32 devices in a mesh: band: 8 (over z, y), sub: 4 (over x, core).
Axes of the slice: x: 2, y: 2, z: 4, core: 2. Of those that a mesh axis runs over, the one named last changes fastest.
Arguments:
- grid_x: bfloat16 [227, 16384], P(None, ('band', 'sub')), may hold values from -6 to 6
- mesh_in: bfloat16 [2048, 512], P(('band', 'sub')), may hold values from -6 to 6
- w_embed: bfloat16 [227, 512], replicated, may hold values from -0.375 to 0.375
- w_src: bfloat16 [512, 512], replicated, may hold values from -0.25 to 0.25
- w_dst: bfloat16 [512, 512], replicated, may hold values from -0.25 to 0.25
- w_edge: bfloat16 [512, 512], replicated, may hold values from -0.25 to 0.25
- w_proc: bfloat16 [512, 512], replicated, may hold values from -0.25 to 0.25
- w_recv: bfloat16 [512, 512], replicated, may hold values from -0.25 to 0.25
- g2m_src: int32 [2048, 40], P(('band', 'sub')), may hold values from 0 to 16383, as said below
- mesh_src: int32 [2048, 6], P(('band', 'sub')), may hold values from 0 to 2047, as said below
- cotangent: bfloat16 [2048, 512], P(('band', 'sub')), may hold values from -6 to 6
Outputs:
- mesh_out: bfloat16 [2048, 512], P(('band', 'sub'))
- grid_grad: float32 [227, 16384], P(None, ('band', 'sub'))
- src_grad: float32 [512, 512], replicated
- edge_grad: float32 [512, 512], replicated
The draws below stay inside these ranges and needn't reach their ends.
Inputs may be any that keep to these rules, and one draw needn't show every extreme that they name: Grid node g belongs to band g // (512 * 4), mesh node m to band m // (64 * 4); g2m_src[m, k] lies in the band of mesh node m, or among the 512 grid nodes of an adjacent band that stand next to that band in index order. mesh_src[m, j] lies in the band of mesh node m, or among the 64 mesh nodes of an adjacent band that stand next to that band in index order.
All inputs are finite; a program needn't handle non-finite values.
Results may differ from the reference program's by a relative error of at most 0.015.
Values may be sent and summed in bfloat16 or wider, within the bound.
A program may use at most 128 MiB of HBM per device.

```python
import math
import jax
import jax.numpy as jnp
from jax import lax

LATENT = 512
CHANNELS = 227
GRID_DEV = 512
MESH_DEV = 64
ENC_EDGES = 40
MESH_EDGES = 6
GRID = 16384
MESH = 2048
N_BAND = 8
N_SUB = 4


def band_sources(key, count, edges, node_dev, source_dev):
    node_band = jnp.arange(count, dtype=jnp.int32) // (node_dev * N_SUB)
    width = source_dev * N_SUB
    total = width * N_BAND
    lowest = jnp.maximum(node_band * width - source_dev, 0)
    highest = jnp.minimum((node_band + 1) * width + source_dev, total)
    return jax.random.randint(key, (count, edges), lowest[:, None], highest[:, None], dtype=jnp.int32)


def draw_g2m_src(key, part):
    return band_sources(jax.random.fold_in(key, 11), MESH, ENC_EDGES, MESH_DEV, GRID_DEV)


def draw_mesh_src(key, part):
    return band_sources(jax.random.fold_in(key, 23), MESH, MESH_EDGES, MESH_DEV, MESH_DEV)


def block_scale(own_key, extent, shards, low, largest):
    gain, own = 1.0, jax.random.fold_in(own_key, 6)
    for position, blocks in shards:
        draws = jnp.exp(jax.random.uniform(jax.random.fold_in(own, position), (blocks,), jnp.float32, low / len(shards), largest / len(shards)))
        gain = gain * jnp.repeat(draws, extent[position] // blocks).reshape([-1 if axis == position else 1 for axis in range(len(extent))])
    return gain


def noise(own_key, shape, scale, reach, shards=(), kind=jnp.bfloat16):
    values = jax.random.normal(own_key, shape, jnp.float32) * scale
    if len(shards) > 0:
        values = block_scale(own_key, shape, shards, -0.22, 0.18) * values
    return jnp.clip(values, min=-reach, max=reach).astype(kind)


def setup_inputs(seed: int = 0) -> dict:
    arg_keys = jax.random.split(jax.random.key(seed), 12)
    return {
        "grid_x": noise(arg_keys[0], (CHANNELS, GRID), 1.0, 6.0, ((1, 32),)),
        "mesh_in": noise(arg_keys[1], (MESH, LATENT), 1.0, 6.0, ((0, 32),)),
        "w_embed": noise(arg_keys[2], (CHANNELS, LATENT), CHANNELS ** -0.5, 0.375),
        "w_src": noise(arg_keys[3], (LATENT, LATENT), LATENT ** -0.5, 0.25),
        "w_dst": noise(arg_keys[4], (LATENT, LATENT), LATENT ** -0.5, 0.25),
        "w_edge": noise(arg_keys[5], (LATENT, LATENT), LATENT ** -0.5, 0.25),
        "w_proc": noise(arg_keys[6], (LATENT, LATENT), LATENT ** -0.5, 0.25),
        "w_recv": noise(arg_keys[7], (LATENT, LATENT), LATENT ** -0.5, 0.25),
        "g2m_src": draw_g2m_src(jax.random.fold_in(arg_keys[11], 71), 0),
        "mesh_src": draw_mesh_src(jax.random.fold_in(arg_keys[11], 71), 0),
        "cotangent": noise(arg_keys[10], (MESH, LATENT), 1.0, 6.0, ((0, 32),)),
    }


EPSILON = 1e-05

def silu_slope(value):
    sigma = jax.nn.sigmoid(value)
    return sigma * (1.0 + value * (1.0 - sigma))

def normalize(value):
    centred = value - lax.optimization_barrier(jnp.mean(value, axis=-1, keepdims=True))
    spread = jnp.sqrt(lax.optimization_barrier(jnp.mean(centred * centred, axis=-1, keepdims=True)) + EPSILON)
    return (centred / spread, spread)

def times_transpose(left, right):
    return lax.dot_general(left, right, (((1,), (1,)), ((), ())), preferred_element_type=jnp.float32)

def first_contract(left, right):
    return lax.dot_general(left, right, (((0,), (0,)), ((), ())), preferred_element_type=jnp.float32)

def encoder_edges(projected, indices, dest_term, w_edge):
    rows = dest_term.shape[0]
    before = jnp.take(projected, indices, axis=0).astype(jnp.float32)
    before = (before.reshape(rows, ENC_EDGES, LATENT) + dest_term[:, None, :]).reshape(rows * ENC_EDGES, LATENT)
    active = jax.nn.silu(before).astype(jnp.bfloat16)
    normed, spread = normalize(jnp.dot(active, w_edge, preferred_element_type=jnp.float32))
    return (before, active, normed, spread)

def reference(grid_x, mesh_in, w_embed, w_src, w_dst, w_edge, w_proc, w_recv, g2m_src, mesh_src, cotangent):
    blocks = MESH // MESH_DEV
    hidden_pre = first_contract(grid_x, w_embed)
    hidden_grid = jax.nn.silu(hidden_pre).astype(jnp.bfloat16)
    projected = jnp.dot(hidden_grid, w_src, preferred_element_type=jnp.float32).astype(jnp.bfloat16)
    dest_term = jnp.dot(mesh_in, w_dst, preferred_element_type=jnp.float32)
    index_blocks = g2m_src.reshape(blocks, MESH_DEV * ENC_EDGES)
    dest_blocks = dest_term.reshape(blocks, MESH_DEV, LATENT)

    def encode(pair):
        before, active, normed, spread = encoder_edges(projected, pair[0], pair[1], w_edge)
        return lax.optimization_barrier(jnp.sum(normed.reshape(MESH_DEV, ENC_EDGES, LATENT), axis=1))
    encoded = lax.map(encode, (index_blocks, dest_blocks)).reshape(MESH, LATENT)
    hidden_mesh = (mesh_in.astype(jnp.float32) + encoded / math.sqrt(ENC_EDGES)).astype(jnp.bfloat16)
    query = jnp.dot(hidden_mesh, w_proc, preferred_element_type=jnp.float32).astype(jnp.bfloat16)
    receiver = jnp.dot(hidden_mesh, w_recv, preferred_element_type=jnp.float32)
    flat_mesh = mesh_src.reshape(-1)
    mesh_before = jnp.take(query, flat_mesh, axis=0).astype(jnp.float32).reshape(MESH, MESH_EDGES, LATENT)
    mesh_before = mesh_before + receiver[:, None, :]
    summed = lax.optimization_barrier(jnp.sum(jax.nn.silu(mesh_before), axis=1))
    mesh_out = (hidden_mesh.astype(jnp.float32) + summed / math.sqrt(MESH_EDGES)).astype(jnp.bfloat16)
    upstream = cotangent.astype(jnp.float32)
    mesh_slope = (upstream / math.sqrt(MESH_EDGES))[:, None, :] * silu_slope(mesh_before)
    receiver_grad = lax.optimization_barrier(jnp.sum(mesh_slope, axis=1))
    query_grad = jnp.zeros((MESH, LATENT), jnp.float32).at[flat_mesh].add(mesh_slope.reshape(-1, LATENT))
    mesh_grad = upstream + times_transpose(query_grad.astype(jnp.bfloat16), w_proc)
    mesh_grad = mesh_grad + times_transpose(receiver_grad.astype(jnp.bfloat16), w_recv)
    grad_blocks = (mesh_grad / math.sqrt(ENC_EDGES)).reshape(blocks, MESH_DEV, LATENT)

    def backward(carry, triple):
        projected_grad, edge_total = carry
        indices, dest, upper = triple
        before, active, normed, spread = encoder_edges(projected, indices, dest, w_edge)
        incoming = jnp.broadcast_to(upper[:, None, :], (MESH_DEV, ENC_EDGES, LATENT)).reshape(-1, LATENT)
        centred_grad = incoming - lax.optimization_barrier(jnp.mean(incoming, axis=-1, keepdims=True))
        centred_grad = centred_grad - normed * lax.optimization_barrier(jnp.mean(incoming * normed, axis=-1, keepdims=True))
        norm_grad = (centred_grad / spread).astype(jnp.bfloat16)
        edge_total = edge_total + first_contract(active, norm_grad)
        before_grad = times_transpose(norm_grad, w_edge) * silu_slope(before)
        projected_grad = projected_grad.at[indices].add(before_grad)
        return ((projected_grad, edge_total), None)
    start = (jnp.zeros((GRID, LATENT), jnp.float32), jnp.zeros((LATENT, LATENT), jnp.float32))
    (projected_grad, edge_grad), _ = lax.scan(backward, start, (index_blocks, dest_blocks, grad_blocks))
    projected_low = projected_grad.astype(jnp.bfloat16)
    src_grad = first_contract(hidden_grid, projected_low)
    hidden_grad = (times_transpose(projected_low, w_src) * silu_slope(hidden_pre)).astype(jnp.bfloat16)
    grid_grad = times_transpose(w_embed, hidden_grad)
    return (mesh_out, grid_grad, src_grad, edge_grad)
```

```python
import functools
import math

import jax
import jax.numpy as jnp
from jax import lax
from jax.experimental import pallas as pl
from jax.experimental.pallas import tpu as pltpu
from jax.sharding import PartitionSpec as P

EPSILON = 1e-05
F32 = jnp.float32
BF16 = jnp.bfloat16
VMEM = pl.BlockSpec(memory_space=pltpu.VMEM)


def silu_slope(value):
    sigma = jax.nn.sigmoid(value)
    return sigma * (1.0 + value * (1.0 - sigma))


def normalize(value):
    centred = value - jnp.mean(value, axis=-1, keepdims=True)
    spread = jnp.sqrt(jnp.mean(centred * centred, axis=-1, keepdims=True) + EPSILON)
    return (centred / spread, spread)


def times_transpose(left, right):
    return lax.dot_general(left, right, (((1,), (1,)), ((), ())), preferred_element_type=F32)


def first_contract(left, right):
    return lax.dot_general(left, right, (((0,), (0,)), ((), ())), preferred_element_type=F32)


def remote(src, dst, send, recv, device):
    return pltpu.make_async_remote_copy(
        src_ref=src,
        dst_ref=dst,
        send_sem=send,
        recv_sem=recv,
        device_id=device,
        device_id_type=pl.DeviceIdType.MESH,
    )


def greet(barrier, device):
    pl.semaphore_signal(barrier, inc=1, device_id=device, device_id_type=pl.DeviceIdType.MESH)


def near_barrier(bands, subs, band, me):
    barrier = pltpu.get_barrier_semaphore()
    for step in range(1, subs):
        greet(barrier, (band, lax.rem(me + step, subs)))

    @pl.when(band > 0)
    def _():
        for other in range(subs):
            greet(barrier, (band - 1, other))

    @pl.when(band < bands - 1)
    def _():
        for other in range(subs):
            greet(barrier, (band + 1, other))

    sides = jnp.minimum(band, 1) + jnp.minimum(bands - 1 - band, 1)
    pl.semaphore_wait(barrier, subs - 1 + subs * sides)


def place(subs):
    band, me = (lax.axis_index("band"), lax.axis_index("sub"))
    core = lax.rem(me, 2)
    return (band, me, core, me // 2, me + 1 - 2 * core, subs // 2)


def window_kernel(bands, subs, x_ref, o_ref, send, recv, local):
    band, me, core, chip, partner, chips = place(subs)
    near_barrier(bands, subs, band, me)
    own = pltpu.make_async_copy(x_ref, o_ref.at[1 + me], local)
    own.start()

    def push(src, slot, b, s, index):
        return remote(src, o_ref.at[slot], send.at[index], recv.at[slot], (b, s))

    def arrived(slot):
        push(x_ref, slot, band, partner, 0).wait_recv()

    across = [
        push(x_ref, 1 + me, band, 2 * lax.rem(chip + k, chips) + core, k - 1)
        for k in range(1, chips)
    ]
    pair = push(x_ref, 1 + me, band, partner, chips - 1)
    rising = (me == subs - 1) & (band < bands - 1)
    falling = (me == 0) & (band > 0)

    def up(k):
        return push(x_ref, 0, band + 1, 2 * k + 1, chips + k)

    def down(k):
        return push(x_ref, subs + 1, band - 1, 2 * k, 2 * chips + k)

    @pl.when(rising)
    def _():
        for k in range(chips):
            up(k).start()

    @pl.when(falling)
    def _():
        for k in range(chips):
            down(k).start()

    for copy in across:
        copy.start()
    pair.start()
    relays = []
    for k in range(1, chips):
        source = lax.rem(chip + chips - k, chips)
        slot = 1 + 2 * source + core
        arrived(slot)
        relay = push(o_ref.at[slot], slot, band, partner, 3 * chips + k - 1)
        relay.start()
        relays.append(relay)

    below = (core == 1) & (band > 0)
    above = (core == 0) & (band < bands - 1)
    relay_below = push(o_ref.at[0], 0, band, partner, 4 * chips - 1)
    relay_above = push(o_ref.at[subs + 1], subs + 1, band, partner, 4 * chips)

    @pl.when(below)
    def _():
        arrived(0)
        relay_below.start()

    @pl.when(above)
    def _():
        arrived(subs + 1)
        relay_above.start()

    @pl.when(band == 0)
    def _():
        o_ref[0] = jnp.zeros(o_ref.shape[1:], o_ref.dtype)

    @pl.when(band == bands - 1)
    def _():
        o_ref[subs + 1] = jnp.zeros(o_ref.shape[1:], o_ref.dtype)

    arrived(1 + partner)
    for k in range(1, chips):
        source = lax.rem(chip + chips - k, chips)
        arrived(2 + 2 * source - core)

    @pl.when((core == 0) & (band > 0))
    def _():
        arrived(0)

    @pl.when((core == 1) & (band < bands - 1))
    def _():
        arrived(subs + 1)

    for copy in across + [pair] + relays:
        copy.wait_send()

    @pl.when(rising)
    def _():
        for k in range(chips):
            up(k).wait_send()

    @pl.when(falling)
    def _():
        for k in range(chips):
            down(k).wait_send()

    @pl.when(below)
    def _():
        relay_below.wait_send()

    @pl.when(above)
    def _():
        relay_above.wait_send()

    own.wait()


def fetch_window(block, bands, subs, ident):
    chips = subs // 2
    return pl.pallas_call(
        functools.partial(window_kernel, bands, subs),
        out_shape=jax.ShapeDtypeStruct((subs + 2,) + block.shape, block.dtype),
        in_specs=[VMEM],
        out_specs=VMEM,
        scratch_shapes=[
            pltpu.SemaphoreType.DMA((4 * chips + 1,)),
            pltpu.SemaphoreType.DMA((subs + 2,)),
            pltpu.SemaphoreType.DMA,
        ],
        compiler_params=pltpu.CompilerParams(collective_id=ident, has_side_effects=True),
        name=f"window{ident}",
    )(block)


def return_kernel(
    bands, subs, g_ref, o_ref, pairbuf, stage, far, edge, send1, recv1, send2, far_sem, edge_sem
):
    band, me, core, chip, partner, chips = place(subs)
    near_barrier(bands, subs, band, me)
    order = list(range(1, chips)) + [chips, 0]

    def slot_of(step, which):
        if step == chips:
            return (1 - which) * (subs + 1)
        return 1 + 2 * lax.rem(chip + step, chips) + which

    swaps = {}
    for step in order:
        swaps[step] = remote(
            g_ref.at[slot_of(step, 1 - core)],
            pairbuf.at[step],
            send1.at[step],
            recv1.at[step],
            (band, partner),
        )
        swaps[step].start()

    def combined(step):
        swaps[step].wait_recv()
        return g_ref[slot_of(step, core)].astype(F32) + pairbuf[step].astype(F32)

    across = []
    for step in range(1, chips):
        stage[step - 1] = combined(step).astype(BF16)
        copy = remote(
            stage.at[step - 1],
            far.at[step - 1],
            send2.at[step - 1],
            far_sem.at[step - 1],
            (band, 2 * lax.rem(chip + step, chips) + core),
        )
        copy.start()
        across.append(copy)
    stage[chips - 1] = combined(chips).astype(BF16)

    def border(b, s):
        return remote(
            stage.at[chips - 1], edge.at[chip], send2.at[chips - 1], edge_sem.at[chip], (b, s)
        )

    below = (core == 1) & (band > 0)
    above = (core == 0) & (band < bands - 1)

    @pl.when(below)
    def _():
        border(band - 1, subs - 1).start()

    @pl.when(above)
    def _():
        border(band + 1, 0).start()

    total = combined(0)
    for step, copy in enumerate(across):
        copy.wait_recv()
        total = total + far[step].astype(F32)
    o_ref[...] = total

    def add_edges():
        extra = o_ref[...]
        for k in range(chips):
            remote(
                stage.at[chips - 1], edge.at[k], send2.at[chips - 1], edge_sem.at[k], (band, partner)
            ).wait_recv()
            extra = extra + edge[k].astype(F32)
        o_ref[...] = extra

    @pl.when((me == subs - 1) & (band < bands - 1))
    def _():
        add_edges()

    @pl.when((me == 0) & (band > 0))
    def _():
        add_edges()

    for step in order:
        swaps[step].wait_send()
    for copy in across:
        copy.wait_send()

    @pl.when(below)
    def _():
        border(band - 1, subs - 1).wait_send()

    @pl.when(above)
    def _():
        border(band + 1, 0).wait_send()


def return_window(slots, bands, subs, ident):
    chips = subs // 2
    block = slots.shape[1:]
    return pl.pallas_call(
        functools.partial(return_kernel, bands, subs),
        out_shape=jax.ShapeDtypeStruct(block, F32),
        in_specs=[VMEM],
        out_specs=VMEM,
        scratch_shapes=[
            pltpu.VMEM((chips + 1,) + block, BF16),
            pltpu.VMEM((chips,) + block, BF16),
            pltpu.VMEM((chips,) + block, BF16),
            pltpu.VMEM((chips,) + block, BF16),
            pltpu.SemaphoreType.DMA((chips + 1,)),
            pltpu.SemaphoreType.DMA((chips + 1,)),
            pltpu.SemaphoreType.DMA((chips,)),
            pltpu.SemaphoreType.DMA((chips,)),
            pltpu.SemaphoreType.DMA((chips,)),
        ],
        compiler_params=pltpu.CompilerParams(collective_id=ident, has_side_effects=True),
        name=f"return{ident}",
    )(slots)


def sum_kernel(
    bands, subs, v_ref, o_ref, r1, a1, r2, a2, r3, s1, q1, s2, q2, s3, q3, s4, q4, s5, q5, s6, q6
):
    band, me, core, chip, partner, chips = place(subs)
    barrier = pltpu.get_barrier_semaphore()
    greet(barrier, (band, partner))
    for k in range(1, chips):
        greet(barrier, (band, 2 * lax.rem(chip + k, chips) + core))
    for i in range(1, bands):
        greet(barrier, (lax.rem(band + i, bands), me))
    pl.semaphore_wait(barrier, chips + bands - 1)
    half = chips * bands

    def part(which, step):
        return pl.ds(which * half + lax.rem(chip + step, chips) * bands, bands)

    order = list(range(1, chips)) + [0]
    swaps = {}
    for step in order:
        swaps[step] = remote(
            v_ref.at[part(1 - core, step)], r1.at[step], s1.at[step], q1.at[step], (band, partner)
        )
        swaps[step].start()
    waits = list(swaps.values())
    across = []
    for step in order:
        swaps[step].wait_recv()
        total = v_ref[part(core, step)].astype(F32) + r1[step].astype(F32)
        if step > 0:
            a1[step] = total.astype(BF16)
            copy = remote(
                a1.at[step],
                r2.at[step],
                s2.at[step],
                q2.at[step],
                (band, 2 * lax.rem(chip + step, chips) + core),
            )
            copy.start()
            across.append(copy)
    for step, copy in enumerate(across):
        copy.wait_recv()
        total = total + r2[step + 1].astype(F32)
    waits += across
    a2[...] = total.astype(BF16)
    spread = []
    for i in range(1, bands):
        goal = lax.rem(band + i, bands)
        copy = remote(a2.at[goal], r3.at[i], s3.at[i], q3.at[i], (goal, me))
        copy.start()
        spread.append(copy)
    total = a2[band].astype(F32)
    for i, copy in enumerate(spread):
        copy.wait_recv()
        total = total + r3[i + 1].astype(F32)
    waits += spread
    mine = core * half + chip * bands + band
    o_ref[mine] = total.astype(BF16)
    spread = []
    for i in range(1, bands):
        copy = remote(
            o_ref.at[mine], o_ref.at[mine], s4.at[i], q4.at[i], (lax.rem(band + i, bands), me)
        )
        copy.start()
        spread.append(copy)
    for copy in spread:
        copy.wait_recv()
    waits += spread
    across = []
    for step in range(1, chips):
        copy = remote(
            o_ref.at[part(core, 0)],
            o_ref.at[part(core, 0)],
            s5.at[step],
            q5.at[step],
            (band, 2 * lax.rem(chip + step, chips) + core),
        )
        copy.start()
        across.append(copy)
    relays = [
        remote(
            o_ref.at[part(core, 0)], o_ref.at[part(core, 0)], s6.at[0], q6.at[0], (band, partner)
        )
    ]
    relays[0].start()
    for step, copy in enumerate(across):
        copy.wait_recv()
        rows = part(core, chips - step - 1)
        relay = remote(
            o_ref.at[rows], o_ref.at[rows], s6.at[step + 1], q6.at[step + 1], (band, partner)
        )
        relay.start()
        relays.append(relay)
    for relay in relays:
        relay.wait_recv()
    for copy in waits + across + relays:
        copy.wait_send()


def sum_all(value, bands, subs, ident):
    chips = subs // 2
    count = bands * subs
    rows, latent = value.shape
    deep = rows // count
    value = value.reshape(count, deep, latent)
    dma = pltpu.SemaphoreType.DMA
    total = pl.pallas_call(
        functools.partial(sum_kernel, bands, subs),
        out_shape=jax.ShapeDtypeStruct(value.shape, BF16),
        in_specs=[VMEM],
        out_specs=VMEM,
        scratch_shapes=[
            pltpu.VMEM((chips, bands, deep, latent), BF16),
            pltpu.VMEM((chips, bands, deep, latent), BF16),
            pltpu.VMEM((chips, bands, deep, latent), BF16),
            pltpu.VMEM((bands, deep, latent), BF16),
            pltpu.VMEM((bands, deep, latent), BF16),
        ]
        + [dma((chips,)), dma((chips,))] * 2
        + [dma((bands,)), dma((bands,))] * 2
        + [dma((chips,)), dma((chips,))] * 2,
        compiler_params=pltpu.CompilerParams(collective_id=ident, has_side_effects=True),
        name=f"sum{ident}",
    )(value)
    return total.reshape(rows, latent)


def one_hot(index, count):
    return (index[:, None] == lax.broadcasted_iota(jnp.int32, (1, count), 1)).astype(BF16)


def body(
    bands, subs,
    grid_x, mesh_in, w_embed, w_src, w_dst, w_edge, w_proc, w_recv, g2m_src, mesh_src, cotangent
):
    latent = w_src.shape[0]
    channels, nodes = grid_x.shape
    mesh_rows, enc_count = g2m_src.shape
    mesh_count = mesh_src.shape[1]
    slots = subs + 2
    band_index = lax.axis_index("band")

    x_window = fetch_window(grid_x, bands, subs, 0)
    hidden_pre = lax.dot_general(
        x_window, w_embed, (((1,), (0,)), ((), ())), preferred_element_type=F32
    ).reshape(slots * nodes, latent)
    hidden = jax.nn.silu(hidden_pre).astype(BF16)
    projected = jnp.dot(hidden, w_src, preferred_element_type=F32).astype(BF16)
    dest_term = jnp.dot(mesh_in, w_dst, preferred_element_type=F32)
    grid_local = (g2m_src - (band_index * (nodes * subs) - nodes)).reshape(-1)
    before = jnp.take(projected, grid_local, axis=0).astype(F32)
    before = (before.reshape(mesh_rows, enc_count, latent) + dest_term[:, None, :]).reshape(
        -1, latent
    )
    active = jax.nn.silu(before).astype(BF16)
    normed, spread = normalize(jnp.dot(active, w_edge, preferred_element_type=F32))
    encoded = jnp.sum(normed.reshape(mesh_rows, enc_count, latent), axis=1)
    hidden_mesh = (mesh_in.astype(F32) + encoded / math.sqrt(enc_count)).astype(BF16)
    query = jnp.dot(hidden_mesh, w_proc, preferred_element_type=F32).astype(BF16)
    receiver = jnp.dot(hidden_mesh, w_recv, preferred_element_type=F32)
    mesh_window = fetch_window(query, bands, subs, 1).reshape(slots * mesh_rows, latent)
    mesh_local = (mesh_src - (band_index * (mesh_rows * subs) - mesh_rows)).T.reshape(-1)
    picks = one_hot(mesh_local, slots * mesh_rows)
    mesh_before = jnp.dot(picks, mesh_window, preferred_element_type=F32)
    mesh_before = mesh_before.reshape(mesh_count, mesh_rows, latent) + receiver[None]
    summed = jnp.sum(jax.nn.silu(mesh_before), axis=0)
    mesh_out = (hidden_mesh.astype(F32) + summed / math.sqrt(mesh_count)).astype(BF16)
    upstream = cotangent.astype(F32)
    mesh_slope = (upstream / math.sqrt(mesh_count))[None] * silu_slope(mesh_before)
    receiver_grad = jnp.sum(mesh_slope, axis=0)
    query_window = first_contract(picks, mesh_slope.reshape(-1, latent).astype(BF16)).astype(BF16)
    query_grad = return_window(query_window.reshape(slots, mesh_rows, latent), bands, subs, 2)
    mesh_grad = upstream + times_transpose(query_grad.astype(BF16), w_proc)
    mesh_grad = mesh_grad + times_transpose(receiver_grad.astype(BF16), w_recv)
    upper = mesh_grad / math.sqrt(enc_count)
    incoming = jnp.broadcast_to(upper[:, None, :], (mesh_rows, enc_count, latent)).reshape(
        -1, latent
    )
    centred_grad = incoming - jnp.mean(incoming, axis=-1, keepdims=True)
    centred_grad = centred_grad - normed * jnp.mean(incoming * normed, axis=-1, keepdims=True)
    norm_grad = (centred_grad / spread).astype(BF16)
    edge_part = first_contract(active, norm_grad)
    before_grad = (times_transpose(norm_grad, w_edge) * silu_slope(before)).astype(BF16)
    window_grad = first_contract(one_hot(grid_local, slots * nodes), before_grad).astype(BF16)
    src_part = first_contract(hidden, window_grad)
    hidden_grad = (times_transpose(window_grad, w_src) * silu_slope(hidden_pre)).astype(BF16)
    grid_part = lax.dot_general(
        w_embed,
        hidden_grad.reshape(slots, nodes, latent),
        (((1,), (2,)), ((), ())),
        preferred_element_type=F32,
    )
    grid_part = jnp.swapaxes(grid_part, 0, 1).astype(BF16)
    grid_grad = return_window(grid_part, bands, subs, 3)
    parts = jnp.concatenate([src_part, edge_part], axis=0).astype(BF16)
    sums = sum_all(parts, bands, subs, 4).astype(F32)
    return (mesh_out, grid_grad, sums[:latent], sums[latent:])


def solution(mesh):
    nodes = P(("band", "sub"), None)
    placed = (P(None, ("band", "sub")), nodes) + (P(),) * 6 + (nodes,) * 3
    return jax.shard_map(
        functools.partial(body, mesh.shape["band"], mesh.shape["sub"]),
        mesh=mesh,
        in_specs=placed,
        out_specs=(nodes, P(None, ("band", "sub")), P(), P()),
        check_vma=False,
    )
```

```python
import functools
import math

import jax
import jax.numpy as jnp
from jax import lax
from jax.experimental import pallas as pl
from jax.experimental.pallas import tpu as pltpu
from jax.sharding import PartitionSpec as P

EPSILON = 1e-05
F32 = jnp.float32
BF16 = jnp.bfloat16
VMEM = pl.BlockSpec(memory_space=pltpu.VMEM)


def silu_slope(value):
    sigma = jax.nn.sigmoid(value)
    return sigma * (1.0 + value * (1.0 - sigma))


def normalize(value):
    centred = value - jnp.mean(value, axis=-1, keepdims=True)
    spread = jnp.sqrt(jnp.mean(centred * centred, axis=-1, keepdims=True) + EPSILON)
    return (centred / spread, spread)


def times_transpose(left, right):
    return lax.dot_general(left, right, (((1,), (1,)), ((), ())), preferred_element_type=F32)


def first_contract(left, right):
    return lax.dot_general(left, right, (((0,), (0,)), ((), ())), preferred_element_type=F32)


def remote(src, dst, send, recv, device):
    return pltpu.make_async_remote_copy(
        src_ref=src,
        dst_ref=dst,
        send_sem=send,
        recv_sem=recv,
        device_id=device,
        device_id_type=pl.DeviceIdType.MESH,
    )


def greet(barrier, device):
    pl.semaphore_signal(barrier, inc=1, device_id=device, device_id_type=pl.DeviceIdType.MESH)


def near_barrier(bands, subs, band, me):
    barrier = pltpu.get_barrier_semaphore()
    for step in range(1, subs):
        greet(barrier, (band, lax.rem(me + step, subs)))

    @pl.when(band > 0)
    def _():
        for other in range(subs):
            greet(barrier, (band - 1, other))

    @pl.when(band < bands - 1)
    def _():
        for other in range(subs):
            greet(barrier, (band + 1, other))

    sides = jnp.minimum(band, 1) + jnp.minimum(bands - 1 - band, 1)
    pl.semaphore_wait(barrier, subs - 1 + subs * sides)


def place(subs):
    band, me = (lax.axis_index("band"), lax.axis_index("sub"))
    core = lax.rem(me, 2)
    return (band, me, core, me // 2, me + 1 - 2 * core, subs // 2)


def window_kernel(bands, subs, x_ref, o_ref, send, recv, local):
    band, me, core, chip, partner, chips = place(subs)
    near_barrier(bands, subs, band, me)
    own = pltpu.make_async_copy(x_ref, o_ref.at[1 + me], local)
    own.start()

    def push(src, slot, b, s, index):
        return remote(src, o_ref.at[slot], send.at[index], recv.at[slot], (b, s))

    def arrived(slot):
        push(x_ref, slot, band, partner, 0).wait_recv()

    across = [
        push(x_ref, 1 + me, band, 2 * lax.rem(chip + k, chips) + core, k - 1)
        for k in range(1, chips)
    ]
    pair = push(x_ref, 1 + me, band, partner, chips - 1)
    rising = (me == subs - 1) & (band < bands - 1)
    falling = (me == 0) & (band > 0)

    def up(k):
        return push(x_ref, 0, band + 1, 2 * k + 1, chips + k)

    def down(k):
        return push(x_ref, subs + 1, band - 1, 2 * k, 2 * chips + k)

    @pl.when(rising)
    def _():
        for k in range(chips):
            up(k).start()

    @pl.when(falling)
    def _():
        for k in range(chips):
            down(k).start()

    for copy in across:
        copy.start()
    pair.start()
    relays = []
    for k in range(1, chips):
        source = lax.rem(chip + chips - k, chips)
        slot = 1 + 2 * source + core
        arrived(slot)
        relay = push(o_ref.at[slot], slot, band, partner, 3 * chips + k - 1)
        relay.start()
        relays.append(relay)

    below = (core == 1) & (band > 0)
    above = (core == 0) & (band < bands - 1)
    relay_below = push(o_ref.at[0], 0, band, partner, 4 * chips - 1)
    relay_above = push(o_ref.at[subs + 1], subs + 1, band, partner, 4 * chips)

    @pl.when(below)
    def _():
        arrived(0)
        relay_below.start()

    @pl.when(above)
    def _():
        arrived(subs + 1)
        relay_above.start()

    @pl.when(band == 0)
    def _():
        o_ref[0] = jnp.zeros(o_ref.shape[1:], o_ref.dtype)

    @pl.when(band == bands - 1)
    def _():
        o_ref[subs + 1] = jnp.zeros(o_ref.shape[1:], o_ref.dtype)

    arrived(1 + partner)
    for k in range(1, chips):
        source = lax.rem(chip + chips - k, chips)
        arrived(2 + 2 * source - core)

    @pl.when((core == 0) & (band > 0))
    def _():
        arrived(0)

    @pl.when((core == 1) & (band < bands - 1))
    def _():
        arrived(subs + 1)

    for copy in across + [pair] + relays:
        copy.wait_send()

    @pl.when(rising)
    def _():
        for k in range(chips):
            up(k).wait_send()

    @pl.when(falling)
    def _():
        for k in range(chips):
            down(k).wait_send()

    @pl.when(below)
    def _():
        relay_below.wait_send()

    @pl.when(above)
    def _():
        relay_above.wait_send()

    own.wait()


def fetch_window(block, bands, subs, ident):
    chips = subs // 2
    return pl.pallas_call(
        functools.partial(window_kernel, bands, subs),
        out_shape=jax.ShapeDtypeStruct((subs + 2,) + block.shape, block.dtype),
        in_specs=[VMEM],
        out_specs=VMEM,
        scratch_shapes=[
            pltpu.SemaphoreType.DMA((4 * chips + 1,)),
            pltpu.SemaphoreType.DMA((subs + 2,)),
            pltpu.SemaphoreType.DMA,
        ],
        compiler_params=pltpu.CompilerParams(collective_id=ident, has_side_effects=True),
        name=f"window{ident}",
    )(block)


def return_stream(
    bands, subs, g_ref, o_ref, pairbuf, stage, far, edge, send1, recv1, send2, far_sem, edge_sem
):
    band, me, core, chip, partner, chips = place(subs)
    order = list(range(1, chips)) + [chips, 0]

    def slot_of(step, which):
        if step == chips:
            return (1 - which) * (subs + 1)
        return 1 + 2 * lax.rem(chip + step, chips) + which

    swaps = {}
    for step in order:
        swaps[step] = remote(
            g_ref.at[slot_of(step, 1 - core)],
            pairbuf.at[step],
            send1.at[step],
            recv1.at[step],
            (band, partner),
        )
        swaps[step].start()
    yield

    def combined(step):
        swaps[step].wait_recv()
        return g_ref[slot_of(step, core)].astype(F32) + pairbuf[step].astype(F32)

    across = []
    for step in range(1, chips):
        stage[step - 1] = combined(step).astype(BF16)
        copy = remote(
            stage.at[step - 1],
            far.at[step - 1],
            send2.at[step - 1],
            far_sem.at[step - 1],
            (band, 2 * lax.rem(chip + step, chips) + core),
        )
        copy.start()
        across.append(copy)
    stage[chips - 1] = combined(chips).astype(BF16)

    def border(b, s):
        return remote(
            stage.at[chips - 1], edge.at[chip], send2.at[chips - 1], edge_sem.at[chip], (b, s)
        )

    below = (core == 1) & (band > 0)
    above = (core == 0) & (band < bands - 1)

    @pl.when(below)
    def _():
        border(band - 1, subs - 1).start()

    @pl.when(above)
    def _():
        border(band + 1, 0).start()

    yield
    total = combined(0)
    for step, copy in enumerate(across):
        copy.wait_recv()
        total = total + far[step].astype(F32)
    o_ref[...] = total

    def add_edges():
        extra = o_ref[...]
        for k in range(chips):
            remote(
                stage.at[chips - 1], edge.at[k], send2.at[chips - 1], edge_sem.at[k], (band, partner)
            ).wait_recv()
            extra = extra + edge[k].astype(F32)
        o_ref[...] = extra

    @pl.when((me == subs - 1) & (band < bands - 1))
    def _():
        add_edges()

    @pl.when((me == 0) & (band > 0))
    def _():
        add_edges()

    for step in order:
        swaps[step].wait_send()
    for copy in across:
        copy.wait_send()

    @pl.when(below)
    def _():
        border(band - 1, subs - 1).wait_send()

    @pl.when(above)
    def _():
        border(band + 1, 0).wait_send()


def return_kernel(bands, subs, *refs):
    band, me = (lax.axis_index("band"), lax.axis_index("sub"))
    near_barrier(bands, subs, band, me)
    for _ in return_stream(bands, subs, *refs):
        pass


def return_scratch(chips, block):
    dma = pltpu.SemaphoreType.DMA
    return [
        pltpu.VMEM((chips + 1,) + block, BF16),
        pltpu.VMEM((chips,) + block, BF16),
        pltpu.VMEM((chips,) + block, BF16),
        pltpu.VMEM((chips,) + block, BF16),
        dma((chips + 1,)),
        dma((chips + 1,)),
        dma((chips,)),
        dma((chips,)),
        dma((chips,)),
    ]


def return_window(slots, bands, subs, ident):
    chips = subs // 2
    block = slots.shape[1:]
    return pl.pallas_call(
        functools.partial(return_kernel, bands, subs),
        out_shape=jax.ShapeDtypeStruct(block, F32),
        in_specs=[VMEM],
        out_specs=VMEM,
        scratch_shapes=return_scratch(chips, block),
        compiler_params=pltpu.CompilerParams(collective_id=ident, has_side_effects=True),
        name=f"return{ident}",
    )(slots)


def sum_stream(
    bands, subs, v_ref, o_ref, r1, a1, r2, a2, r3, s1, q1, s2, q2, s3, q3, s4, q4, s5, q5, s6, q6
):
    band, me, core, chip, partner, chips = place(subs)
    half = chips * bands

    def part(which, step):
        return pl.ds(which * half + lax.rem(chip + step, chips) * bands, bands)

    order = list(range(1, chips)) + [0]
    swaps = {}
    for step in order:
        swaps[step] = remote(
            v_ref.at[part(1 - core, step)], r1.at[step], s1.at[step], q1.at[step], (band, partner)
        )
        swaps[step].start()
    waits = list(swaps.values())
    yield
    across = []
    for step in order:
        swaps[step].wait_recv()
        total = v_ref[part(core, step)].astype(F32) + r1[step].astype(F32)
        if step > 0:
            a1[step] = total.astype(BF16)
            copy = remote(
                a1.at[step],
                r2.at[step],
                s2.at[step],
                q2.at[step],
                (band, 2 * lax.rem(chip + step, chips) + core),
            )
            copy.start()
            across.append(copy)
    yield
    for step, copy in enumerate(across):
        copy.wait_recv()
        total = total + r2[step + 1].astype(F32)
    waits += across
    a2[...] = total.astype(BF16)
    spread = []
    for i in range(1, bands):
        goal = lax.rem(band + i, bands)
        copy = remote(a2.at[goal], r3.at[i], s3.at[i], q3.at[i], (goal, me))
        copy.start()
        spread.append(copy)
    yield
    total = a2[band].astype(F32)
    for i, copy in enumerate(spread):
        copy.wait_recv()
        total = total + r3[i + 1].astype(F32)
    waits += spread
    mine = core * half + chip * bands + band
    o_ref[mine] = total.astype(BF16)
    spread = []
    for i in range(1, bands):
        copy = remote(
            o_ref.at[mine], o_ref.at[mine], s4.at[i], q4.at[i], (lax.rem(band + i, bands), me)
        )
        copy.start()
        spread.append(copy)
    yield
    for copy in spread:
        copy.wait_recv()
    waits += spread
    across = []
    for step in range(1, chips):
        copy = remote(
            o_ref.at[part(core, 0)],
            o_ref.at[part(core, 0)],
            s5.at[step],
            q5.at[step],
            (band, 2 * lax.rem(chip + step, chips) + core),
        )
        copy.start()
        across.append(copy)
    relays = [
        remote(
            o_ref.at[part(core, 0)], o_ref.at[part(core, 0)], s6.at[0], q6.at[0], (band, partner)
        )
    ]
    relays[0].start()
    yield
    for step, copy in enumerate(across):
        copy.wait_recv()
        rows = part(core, chips - step - 1)
        relay = remote(
            o_ref.at[rows], o_ref.at[rows], s6.at[step + 1], q6.at[step + 1], (band, partner)
        )
        relay.start()
        relays.append(relay)
    yield
    for relay in relays:
        relay.wait_recv()
    for copy in waits + across + relays:
        copy.wait_send()


def sum_scratch(chips, bands, deep, latent):
    dma = pltpu.SemaphoreType.DMA
    return (
        [pltpu.VMEM((chips, bands, deep, latent), BF16)] * 3
        + [pltpu.VMEM((bands, deep, latent), BF16)] * 2
        + [dma((chips,))] * 4
        + [dma((bands,))] * 4
        + [dma((chips,))] * 4
    )


def tail_kernel(bands, subs, streams, *refs):
    band, me = (lax.axis_index("band"), lax.axis_index("sub"))
    barrier = pltpu.get_barrier_semaphore()
    for step in range(1, subs):
        greet(barrier, (band, lax.rem(me + step, subs)))

    @pl.when(band > 0)
    def _():
        for other in range(subs):
            greet(barrier, (band - 1, other))

    @pl.when(band < bands - 1)
    def _():
        for other in range(subs):
            greet(barrier, (band + 1, other))

    for i in range(1, bands):
        goal = lax.rem(band + i, bands)

        @pl.when((goal != band + 1) & (goal != band - 1))
        def _():
            greet(barrier, (goal, me))

    sides = jnp.minimum(band, 1) + jnp.minimum(bands - 1 - band, 1)
    pl.semaphore_wait(barrier, subs + bands - 2 + (subs - 1) * sides)
    count = streams + 1
    ins, outs, scratch = (refs[:count], refs[count : 2 * count], refs[2 * count :])
    active = [
        sum_stream(bands, subs, ins[i], outs[i], *scratch[17 * i : 17 * i + 17])
        for i in range(streams)
    ]
    active.append(return_stream(bands, subs, ins[-1], outs[-1], *scratch[17 * streams :]))
    while active:
        active = [stream for stream in active if next(stream, True) is None]


def tail(values, slots, bands, subs, ident):
    chips = subs // 2
    count = bands * subs
    rows, latent = values[0].shape
    deep = rows // count
    block = slots.shape[1:]
    shape = (count, deep, latent)
    scratch = []
    for _ in values:
        scratch += sum_scratch(chips, bands, deep, latent)
    results = pl.pallas_call(
        functools.partial(tail_kernel, bands, subs, len(values)),
        out_shape=[jax.ShapeDtypeStruct(shape, BF16)] * len(values)
        + [jax.ShapeDtypeStruct(block, F32)],
        in_specs=[VMEM] * (len(values) + 1),
        out_specs=[VMEM] * (len(values) + 1),
        scratch_shapes=scratch + return_scratch(chips, block),
        compiler_params=pltpu.CompilerParams(collective_id=ident, has_side_effects=True),
        name="tail",
    )(*[value.reshape(shape) for value in values], slots)
    return [result.reshape(rows, latent) for result in results[:-1]] + [results[-1]]


def one_hot(index, count):
    return (index[:, None] == lax.broadcasted_iota(jnp.int32, (1, count), 1)).astype(BF16)


def body(
    bands, subs,
    grid_x, mesh_in, w_embed, w_src, w_dst, w_edge, w_proc, w_recv, g2m_src, mesh_src, cotangent
):
    latent = w_src.shape[0]
    channels, nodes = grid_x.shape
    mesh_rows, enc_count = g2m_src.shape
    mesh_count = mesh_src.shape[1]
    slots = subs + 2
    band_index = lax.axis_index("band")

    x_window = fetch_window(grid_x, bands, subs, 0)
    hidden_pre = lax.dot_general(
        x_window, w_embed, (((1,), (0,)), ((), ())), preferred_element_type=F32
    ).reshape(slots * nodes, latent)
    hidden = jax.nn.silu(hidden_pre).astype(BF16)
    projected = jnp.dot(hidden, w_src, preferred_element_type=F32).astype(BF16)
    dest_term = jnp.dot(mesh_in, w_dst, preferred_element_type=F32)
    grid_local = (g2m_src - (band_index * (nodes * subs) - nodes)).reshape(-1)
    before = jnp.take(projected, grid_local, axis=0).astype(F32)
    before = (before.reshape(mesh_rows, enc_count, latent) + dest_term[:, None, :]).reshape(
        -1, latent
    )
    active = jax.nn.silu(before).astype(BF16)
    normed, spread = normalize(jnp.dot(active, w_edge, preferred_element_type=F32))
    encoded = jnp.sum(normed.reshape(mesh_rows, enc_count, latent), axis=1)
    hidden_mesh = (mesh_in.astype(F32) + encoded / math.sqrt(enc_count)).astype(BF16)
    query = jnp.dot(hidden_mesh, w_proc, preferred_element_type=F32).astype(BF16)
    receiver = jnp.dot(hidden_mesh, w_recv, preferred_element_type=F32)
    mesh_window = fetch_window(query, bands, subs, 1).reshape(slots * mesh_rows, latent)
    mesh_local = (mesh_src - (band_index * (mesh_rows * subs) - mesh_rows)).T.reshape(-1)
    picks = one_hot(mesh_local, slots * mesh_rows)
    mesh_before = jnp.dot(picks, mesh_window, preferred_element_type=F32)
    mesh_before = mesh_before.reshape(mesh_count, mesh_rows, latent) + receiver[None]
    summed = jnp.sum(jax.nn.silu(mesh_before), axis=0)
    mesh_out = (hidden_mesh.astype(F32) + summed / math.sqrt(mesh_count)).astype(BF16)
    upstream = cotangent.astype(F32)
    mesh_slope = (upstream / math.sqrt(mesh_count))[None] * silu_slope(mesh_before)
    receiver_grad = jnp.sum(mesh_slope, axis=0)
    query_window = first_contract(picks, mesh_slope.reshape(-1, latent).astype(BF16)).astype(BF16)
    query_grad = return_window(query_window.reshape(slots, mesh_rows, latent), bands, subs, 2)
    mesh_grad = upstream + times_transpose(query_grad.astype(BF16), w_proc)
    mesh_grad = mesh_grad + times_transpose(receiver_grad.astype(BF16), w_recv)
    upper = mesh_grad / math.sqrt(enc_count)
    incoming = jnp.broadcast_to(upper[:, None, :], (mesh_rows, enc_count, latent)).reshape(
        -1, latent
    )
    centred_grad = incoming - jnp.mean(incoming, axis=-1, keepdims=True)
    centred_grad = centred_grad - normed * jnp.mean(incoming * normed, axis=-1, keepdims=True)
    norm_grad = (centred_grad / spread).astype(BF16)
    edge_part = first_contract(active, norm_grad)
    before_grad = (times_transpose(norm_grad, w_edge) * silu_slope(before)).astype(BF16)
    window_grad = first_contract(one_hot(grid_local, slots * nodes), before_grad).astype(BF16)
    src_part = first_contract(hidden, window_grad)
    hidden_grad = (times_transpose(window_grad, w_src) * silu_slope(hidden_pre)).astype(BF16)
    grid_part = lax.dot_general(
        w_embed,
        hidden_grad.reshape(slots, nodes, latent),
        (((1,), (2,)), ((), ())),
        preferred_element_type=F32,
    )
    grid_part = jnp.swapaxes(grid_part, 0, 1).astype(BF16)
    src_grad, edge_grad, grid_grad = tail(
        [src_part.astype(BF16), edge_part.astype(BF16)], grid_part, bands, subs, 3
    )
    return (mesh_out, grid_grad, src_grad.astype(F32), edge_grad.astype(F32))


def solution(mesh):
    nodes = P(("band", "sub"), None)
    placed = (P(None, ("band", "sub")), nodes) + (P(),) * 6 + (nodes,) * 3
    return jax.shard_map(
        functools.partial(body, mesh.shape["band"], mesh.shape["sub"]),
        mesh=mesh,
        in_specs=placed,
        out_specs=(nodes, P(None, ("band", "sub")), P(), P()),
        check_vma=False,
    )
```

```python
import functools
import math

import jax
import jax.numpy as jnp
from jax import lax
from jax.experimental import pallas as pl
from jax.experimental.pallas import tpu as pltpu
from jax.sharding import PartitionSpec as P

EPSILON = 1e-05
F32 = jnp.float32
BF16 = jnp.bfloat16
VMEM = pl.BlockSpec(memory_space=pltpu.VMEM)


def silu_slope(value):
    sigma = jax.nn.sigmoid(value)
    return sigma * (1.0 + value * (1.0 - sigma))


def times_transpose(left, right):
    return lax.dot_general(left, right, (((1,), (1,)), ((), ())), preferred_element_type=F32)


def first_contract(left, right):
    return lax.dot_general(left, right, (((0,), (0,)), ((), ())), preferred_element_type=F32)


def remote(src, dst, send, recv, device):
    return pltpu.make_async_remote_copy(
        src_ref=src,
        dst_ref=dst,
        send_sem=send,
        recv_sem=recv,
        device_id=device,
        device_id_type=pl.DeviceIdType.MESH,
    )


def greet(barrier, device):
    pl.semaphore_signal(barrier, inc=1, device_id=device, device_id_type=pl.DeviceIdType.MESH)


def near_barrier(bands, subs, band, me):
    barrier = pltpu.get_barrier_semaphore()
    for step in range(1, subs):
        greet(barrier, (band, lax.rem(me + step, subs)))

    @pl.when(band > 0)
    def _():
        for other in range(subs):
            greet(barrier, (band - 1, other))

    @pl.when(band < bands - 1)
    def _():
        for other in range(subs):
            greet(barrier, (band + 1, other))

    sides = jnp.minimum(band, 1) + jnp.minimum(bands - 1 - band, 1)
    pl.semaphore_wait(barrier, subs - 1 + subs * sides)


def place(subs):
    band, me = (lax.axis_index("band"), lax.axis_index("sub"))
    core = lax.rem(me, 2)
    return (band, me, core, me // 2, me + 1 - 2 * core, subs // 2)


def window_kernel(bands, subs, x_ref, o_ref, send, recv, local):
    band, me, core, chip, partner, chips = place(subs)
    near_barrier(bands, subs, band, me)
    own = pltpu.make_async_copy(x_ref, o_ref.at[1 + me], local)
    own.start()

    def push(src, slot, b, s, index):
        return remote(src, o_ref.at[slot], send.at[index], recv.at[slot], (b, s))

    def arrived(slot):
        push(x_ref, slot, band, partner, 0).wait_recv()

    across = [
        push(x_ref, 1 + me, band, 2 * lax.rem(chip + k, chips) + core, k - 1)
        for k in range(1, chips)
    ]
    pair = push(x_ref, 1 + me, band, partner, chips - 1)
    rising = (me == subs - 1) & (band < bands - 1)
    falling = (me == 0) & (band > 0)

    def up(k):
        return push(x_ref, 0, band + 1, 2 * k + 1, chips + k)

    def down(k):
        return push(x_ref, subs + 1, band - 1, 2 * k, 2 * chips + k)

    @pl.when(rising)
    def _():
        for k in range(chips):
            up(k).start()

    @pl.when(falling)
    def _():
        for k in range(chips):
            down(k).start()

    for copy in across:
        copy.start()
    pair.start()
    relays = []
    for k in range(1, chips):
        source = lax.rem(chip + chips - k, chips)
        slot = 1 + 2 * source + core
        arrived(slot)
        relay = push(o_ref.at[slot], slot, band, partner, 3 * chips + k - 1)
        relay.start()
        relays.append(relay)

    below = (core == 1) & (band > 0)
    above = (core == 0) & (band < bands - 1)
    relay_below = push(o_ref.at[0], 0, band, partner, 4 * chips - 1)
    relay_above = push(o_ref.at[subs + 1], subs + 1, band, partner, 4 * chips)

    @pl.when(below)
    def _():
        arrived(0)
        relay_below.start()

    @pl.when(above)
    def _():
        arrived(subs + 1)
        relay_above.start()

    @pl.when(band == 0)
    def _():
        o_ref[0] = jnp.zeros(o_ref.shape[1:], o_ref.dtype)

    @pl.when(band == bands - 1)
    def _():
        o_ref[subs + 1] = jnp.zeros(o_ref.shape[1:], o_ref.dtype)

    arrived(1 + partner)
    for k in range(1, chips):
        source = lax.rem(chip + chips - k, chips)
        arrived(2 + 2 * source - core)

    @pl.when((core == 0) & (band > 0))
    def _():
        arrived(0)

    @pl.when((core == 1) & (band < bands - 1))
    def _():
        arrived(subs + 1)

    for copy in across + [pair] + relays:
        copy.wait_send()

    @pl.when(rising)
    def _():
        for k in range(chips):
            up(k).wait_send()

    @pl.when(falling)
    def _():
        for k in range(chips):
            down(k).wait_send()

    @pl.when(below)
    def _():
        relay_below.wait_send()

    @pl.when(above)
    def _():
        relay_above.wait_send()

    own.wait()


def fetch_window(block, bands, subs, ident):
    chips = subs // 2
    return pl.pallas_call(
        functools.partial(window_kernel, bands, subs),
        out_shape=jax.ShapeDtypeStruct((subs + 2,) + block.shape, block.dtype),
        in_specs=[VMEM],
        out_specs=VMEM,
        scratch_shapes=[
            pltpu.SemaphoreType.DMA((4 * chips + 1,)),
            pltpu.SemaphoreType.DMA((subs + 2,)),
            pltpu.SemaphoreType.DMA,
        ],
        compiler_params=pltpu.CompilerParams(collective_id=ident, has_side_effects=True),
        name=f"window{ident}",
    )(block)


def return_stream(
    bands, subs, g_ref, o_ref, pairbuf, stage, far, edge, send1, recv1, send2, far_sem, edge_sem
):
    band, me, core, chip, partner, chips = place(subs)
    order = list(range(1, chips)) + [chips, 0]

    def slot_of(step, which):
        if step == chips:
            return (1 - which) * (subs + 1)
        return 1 + 2 * lax.rem(chip + step, chips) + which

    swaps = {}
    for step in order:
        swaps[step] = remote(
            g_ref.at[slot_of(step, 1 - core)],
            pairbuf.at[step],
            send1.at[step],
            recv1.at[step],
            (band, partner),
        )
        swaps[step].start()
    yield

    def combined(step):
        swaps[step].wait_recv()
        return g_ref[slot_of(step, core)].astype(F32) + pairbuf[step].astype(F32)

    across = []
    for step in range(1, chips):
        stage[step - 1] = combined(step).astype(BF16)
        copy = remote(
            stage.at[step - 1],
            far.at[step - 1],
            send2.at[step - 1],
            far_sem.at[step - 1],
            (band, 2 * lax.rem(chip + step, chips) + core),
        )
        copy.start()
        across.append(copy)
    stage[chips - 1] = combined(chips).astype(BF16)

    def border(b, s):
        return remote(
            stage.at[chips - 1], edge.at[chip], send2.at[chips - 1], edge_sem.at[chip], (b, s)
        )

    below = (core == 1) & (band > 0)
    above = (core == 0) & (band < bands - 1)

    @pl.when(below)
    def _():
        border(band - 1, subs - 1).start()

    @pl.when(above)
    def _():
        border(band + 1, 0).start()

    yield
    total = combined(0)
    for step, copy in enumerate(across):
        copy.wait_recv()
        total = total + far[step].astype(F32)
    o_ref[...] = total

    def add_edges():
        extra = o_ref[...]
        for k in range(chips):
            remote(
                stage.at[chips - 1], edge.at[k], send2.at[chips - 1], edge_sem.at[k], (band, partner)
            ).wait_recv()
            extra = extra + edge[k].astype(F32)
        o_ref[...] = extra

    @pl.when((me == subs - 1) & (band < bands - 1))
    def _():
        add_edges()

    @pl.when((me == 0) & (band > 0))
    def _():
        add_edges()

    for step in order:
        swaps[step].wait_send()
    for copy in across:
        copy.wait_send()

    @pl.when(below)
    def _():
        border(band - 1, subs - 1).wait_send()

    @pl.when(above)
    def _():
        border(band + 1, 0).wait_send()


def return_kernel(bands, subs, *refs):
    band, me = (lax.axis_index("band"), lax.axis_index("sub"))
    near_barrier(bands, subs, band, me)
    for _ in return_stream(bands, subs, *refs):
        pass


def return_scratch(chips, block):
    dma = pltpu.SemaphoreType.DMA
    return [
        pltpu.VMEM((chips + 1,) + block, BF16),
        pltpu.VMEM((chips,) + block, BF16),
        pltpu.VMEM((chips,) + block, BF16),
        pltpu.VMEM((chips,) + block, BF16),
        dma((chips + 1,)),
        dma((chips + 1,)),
        dma((chips,)),
        dma((chips,)),
        dma((chips,)),
    ]


def return_window(slots, bands, subs, ident):
    chips = subs // 2
    block = slots.shape[1:]
    return pl.pallas_call(
        functools.partial(return_kernel, bands, subs),
        out_shape=jax.ShapeDtypeStruct(block, F32),
        in_specs=[VMEM],
        out_specs=VMEM,
        scratch_shapes=return_scratch(chips, block),
        compiler_params=pltpu.CompilerParams(collective_id=ident, has_side_effects=True),
        name=f"return{ident}",
    )(slots)


def sum_stream(
    bands, subs, v_ref, o_ref, r1, a1, r2, a2, r3, s1, q1, s2, q2, s3, q3, s4, q4, s5, q5, s6, q6
):
    band, me, core, chip, partner, chips = place(subs)
    half = chips * bands

    def part(which, step):
        return pl.ds(which * half + lax.rem(chip + step, chips) * bands, bands)

    order = list(range(1, chips)) + [0]
    swaps = {}
    for step in order:
        swaps[step] = remote(
            v_ref.at[part(1 - core, step)], r1.at[step], s1.at[step], q1.at[step], (band, partner)
        )
        swaps[step].start()
    waits = list(swaps.values())
    yield
    across = []
    for step in order:
        swaps[step].wait_recv()
        total = v_ref[part(core, step)].astype(F32) + r1[step].astype(F32)
        if step > 0:
            a1[step] = total.astype(BF16)
            copy = remote(
                a1.at[step],
                r2.at[step],
                s2.at[step],
                q2.at[step],
                (band, 2 * lax.rem(chip + step, chips) + core),
            )
            copy.start()
            across.append(copy)
    yield
    for step, copy in enumerate(across):
        copy.wait_recv()
        total = total + r2[step + 1].astype(F32)
    waits += across
    a2[...] = total.astype(BF16)
    spread = []
    for i in range(1, bands):
        goal = lax.rem(band + i, bands)
        copy = remote(a2.at[goal], r3.at[i], s3.at[i], q3.at[i], (goal, me))
        copy.start()
        spread.append(copy)
    yield
    total = a2[band].astype(F32)
    for i, copy in enumerate(spread):
        copy.wait_recv()
        total = total + r3[i + 1].astype(F32)
    waits += spread
    mine = core * half + chip * bands + band
    o_ref[mine] = total.astype(BF16)
    spread = []
    for i in range(1, bands):
        copy = remote(
            o_ref.at[mine], o_ref.at[mine], s4.at[i], q4.at[i], (lax.rem(band + i, bands), me)
        )
        copy.start()
        spread.append(copy)
    yield
    for copy in spread:
        copy.wait_recv()
    waits += spread
    across = []
    for step in range(1, chips):
        copy = remote(
            o_ref.at[part(core, 0)],
            o_ref.at[part(core, 0)],
            s5.at[step],
            q5.at[step],
            (band, 2 * lax.rem(chip + step, chips) + core),
        )
        copy.start()
        across.append(copy)
    relays = [
        remote(
            o_ref.at[part(core, 0)], o_ref.at[part(core, 0)], s6.at[0], q6.at[0], (band, partner)
        )
    ]
    relays[0].start()
    yield
    for step, copy in enumerate(across):
        copy.wait_recv()
        rows = part(core, chips - step - 1)
        relay = remote(
            o_ref.at[rows], o_ref.at[rows], s6.at[step + 1], q6.at[step + 1], (band, partner)
        )
        relay.start()
        relays.append(relay)
    yield
    for relay in relays:
        relay.wait_recv()
    for copy in waits + across + relays:
        copy.wait_send()


def sum_scratch(chips, bands, deep, latent):
    dma = pltpu.SemaphoreType.DMA
    return (
        [pltpu.VMEM((chips, bands, deep, latent), BF16)] * 3
        + [pltpu.VMEM((bands, deep, latent), BF16)] * 2
        + [dma((chips,))] * 4
        + [dma((bands,))] * 4
        + [dma((chips,))] * 4
    )


def tail_kernel(bands, subs, streams, *refs):
    band, me = (lax.axis_index("band"), lax.axis_index("sub"))
    barrier = pltpu.get_barrier_semaphore()
    for step in range(1, subs):
        greet(barrier, (band, lax.rem(me + step, subs)))

    @pl.when(band > 0)
    def _():
        for other in range(subs):
            greet(barrier, (band - 1, other))

    @pl.when(band < bands - 1)
    def _():
        for other in range(subs):
            greet(barrier, (band + 1, other))

    for i in range(1, bands):
        goal = lax.rem(band + i, bands)

        @pl.when((goal != band + 1) & (goal != band - 1))
        def _():
            greet(barrier, (goal, me))

    sides = jnp.minimum(band, 1) + jnp.minimum(bands - 1 - band, 1)
    pl.semaphore_wait(barrier, subs + bands - 2 + (subs - 1) * sides)
    count = streams + 1
    ins, outs, scratch = (refs[:count], refs[count : 2 * count], refs[2 * count :])
    active = [
        sum_stream(bands, subs, ins[i], outs[i], *scratch[17 * i : 17 * i + 17])
        for i in range(streams)
    ]
    active.append(return_stream(bands, subs, ins[-1], outs[-1], *scratch[17 * streams :]))
    while active:
        active = [stream for stream in active if next(stream, True) is None]


def tail(values, slots, bands, subs, ident):
    chips = subs // 2
    count = bands * subs
    rows, latent = values[0].shape
    deep = rows // count
    block = slots.shape[1:]
    shape = (count, deep, latent)
    scratch = []
    for _ in values:
        scratch += sum_scratch(chips, bands, deep, latent)
    results = pl.pallas_call(
        functools.partial(tail_kernel, bands, subs, len(values)),
        out_shape=[jax.ShapeDtypeStruct(shape, BF16)] * len(values)
        + [jax.ShapeDtypeStruct(block, F32)],
        in_specs=[VMEM] * (len(values) + 1),
        out_specs=[VMEM] * (len(values) + 1),
        scratch_shapes=scratch + return_scratch(chips, block),
        compiler_params=pltpu.CompilerParams(collective_id=ident, has_side_effects=True),
        name="tail",
    )(*[value.reshape(shape) for value in values], slots)
    return [result.reshape(rows, latent) for result in results[:-1]] + [results[-1]]


def encode_kernel(edges, g_ref, d_ref, m_ref, w_ref, a_ref, l_ref, n_ref, i_ref, h_ref):
    rows, latent = d_ref.shape
    before = g_ref[...].astype(F32).reshape(rows, edges, latent) + d_ref[...][:, None, :]
    before = before.reshape(rows * edges, latent)
    sigma = jax.nn.sigmoid(before)
    active = before * sigma
    l_ref[...] = (sigma + active * (1.0 - sigma)).astype(BF16)
    active = active.astype(BF16)
    a_ref[...] = active
    out = jnp.dot(active, w_ref[...], preferred_element_type=F32)
    out = out - jnp.mean(out, axis=-1, keepdims=True)
    inverse = 1.0 / jnp.sqrt(jnp.mean(out * out, axis=-1, keepdims=True) + EPSILON)
    out = out * inverse
    i_ref[...] = inverse
    n_ref[...] = out.astype(BF16)
    encoded = jnp.sum(out.reshape(rows, edges, latent), axis=1)
    h_ref[...] = (m_ref[...].astype(F32) + encoded * (1.0 / math.sqrt(edges))).astype(BF16)


def rows_spec(rows, width):
    return pl.BlockSpec((rows, width), lambda i: (i, 0))


def encode(gathered, dest, mesh_in, w_edge, edges, tile):
    rows, latent = dest.shape
    total = rows * edges
    wide = rows_spec(tile * edges, latent)
    return pl.pallas_call(
        functools.partial(encode_kernel, edges),
        grid=(rows // tile,),
        out_shape=[jax.ShapeDtypeStruct((total, latent), BF16)] * 3
        + [
            jax.ShapeDtypeStruct((total, 1), F32),
            jax.ShapeDtypeStruct((rows, latent), BF16),
        ],
        in_specs=[
            wide,
            rows_spec(tile, latent),
            rows_spec(tile, latent),
            pl.BlockSpec((latent, latent), lambda i: (0, 0)),
        ],
        out_specs=[wide] * 3 + [rows_spec(tile * edges, 1), rows_spec(tile, latent)],
        name="encode",
    )(gathered, dest, mesh_in, w_edge)


def decode_kernel(edges, u_ref, n_ref, i_ref, l_ref, w_ref, g_ref, b_ref):
    rows, latent = u_ref.shape
    upper = u_ref[...] * (1.0 / math.sqrt(edges))
    normed = n_ref[...].astype(F32).reshape(rows, edges, latent)
    both = jnp.mean(upper[:, None, :] * normed, axis=-1, keepdims=True)
    upper = upper - jnp.mean(upper, axis=-1, keepdims=True)
    grad = (upper[:, None, :] - normed * both).reshape(rows * edges, latent) * i_ref[...]
    grad = grad.astype(BF16)
    g_ref[...] = grad
    b_ref[...] = (times_transpose(grad, w_ref[...]) * l_ref[...].astype(F32)).astype(BF16)


def decode(mesh_grad, normed, inverse, slope, w_edge, edges, tile):
    rows, latent = mesh_grad.shape
    wide = rows_spec(tile * edges, latent)
    return pl.pallas_call(
        functools.partial(decode_kernel, edges),
        grid=(rows // tile,),
        out_shape=[jax.ShapeDtypeStruct((rows * edges, latent), BF16)] * 2,
        in_specs=[
            rows_spec(tile, latent),
            wide,
            rows_spec(tile * edges, 1),
            wide,
            pl.BlockSpec((latent, latent), lambda i: (0, 0)),
        ],
        out_specs=[wide] * 2,
        name="decode",
    )(mesh_grad, normed, inverse, slope, w_edge)


def one_hot(index, count):
    return (index[:, None] == lax.broadcasted_iota(jnp.int32, (1, count), 1)).astype(BF16)


def body(
    bands, subs,
    grid_x, mesh_in, w_embed, w_src, w_dst, w_edge, w_proc, w_recv, g2m_src, mesh_src, cotangent
):
    latent = w_src.shape[0]
    channels, nodes = grid_x.shape
    mesh_rows, enc_count = g2m_src.shape
    mesh_count = mesh_src.shape[1]
    slots = subs + 2
    band_index = lax.axis_index("band")

    x_window = fetch_window(grid_x, bands, subs, 0)
    hidden_pre = lax.dot_general(
        x_window, w_embed, (((1,), (0,)), ((), ())), preferred_element_type=F32
    ).reshape(slots * nodes, latent)
    hidden = jax.nn.silu(hidden_pre).astype(BF16)
    projected = jnp.dot(hidden, w_src, preferred_element_type=F32).astype(BF16)
    dest_term = jnp.dot(mesh_in, w_dst, preferred_element_type=F32)
    grid_local = (g2m_src - (band_index * (nodes * subs) - nodes)).reshape(-1)
    gathered = jnp.take(projected, grid_local, axis=0)
    active, slope, normed, inverse, hidden_mesh = encode(
        gathered, dest_term, mesh_in, w_edge, enc_count, 16
    )
    query = jnp.dot(hidden_mesh, w_proc, preferred_element_type=F32).astype(BF16)
    receiver = jnp.dot(hidden_mesh, w_recv, preferred_element_type=F32)
    mesh_window = fetch_window(query, bands, subs, 1).reshape(slots * mesh_rows, latent)
    mesh_local = (mesh_src - (band_index * (mesh_rows * subs) - mesh_rows)).T.reshape(-1)
    picks = one_hot(mesh_local, slots * mesh_rows)
    mesh_before = jnp.dot(picks, mesh_window, preferred_element_type=F32)
    mesh_before = mesh_before.reshape(mesh_count, mesh_rows, latent) + receiver[None]
    summed = jnp.sum(jax.nn.silu(mesh_before), axis=0)
    mesh_out = (hidden_mesh.astype(F32) + summed / math.sqrt(mesh_count)).astype(BF16)
    upstream = cotangent.astype(F32)
    mesh_slope = (upstream / math.sqrt(mesh_count))[None] * silu_slope(mesh_before)
    receiver_grad = jnp.sum(mesh_slope, axis=0)
    query_window = first_contract(picks, mesh_slope.reshape(-1, latent).astype(BF16)).astype(BF16)
    query_grad = return_window(query_window.reshape(slots, mesh_rows, latent), bands, subs, 2)
    mesh_grad = upstream + times_transpose(query_grad.astype(BF16), w_proc)
    mesh_grad = mesh_grad + times_transpose(receiver_grad.astype(BF16), w_recv)
    norm_grad, before_grad = decode(mesh_grad, normed, inverse, slope, w_edge, enc_count, 16)
    edge_part = first_contract(active, norm_grad)
    window_grad = first_contract(one_hot(grid_local, slots * nodes), before_grad).astype(BF16)
    src_part = first_contract(hidden, window_grad)
    hidden_grad = (times_transpose(window_grad, w_src) * silu_slope(hidden_pre)).astype(BF16)
    grid_part = lax.dot_general(
        w_embed,
        hidden_grad.reshape(slots, nodes, latent),
        (((1,), (2,)), ((), ())),
        preferred_element_type=F32,
    )
    grid_part = jnp.swapaxes(grid_part, 0, 1).astype(BF16)
    src_grad, edge_grad, grid_grad = tail(
        [src_part.astype(BF16), edge_part.astype(BF16)], grid_part, bands, subs, 3
    )
    return (mesh_out, grid_grad, src_grad.astype(F32), edge_grad.astype(F32))


def solution(mesh):
    nodes = P(("band", "sub"), None)
    placed = (P(None, ("band", "sub")), nodes) + (P(),) * 6 + (nodes,) * 3
    return jax.shard_map(
        functools.partial(body, mesh.shape["band"], mesh.shape["sub"]),
        mesh=mesh,
        in_specs=placed,
        out_specs=(nodes, P(None, ("band", "sub")), P(), P()),
        check_vma=False,
    )
```

```python
import functools
import math

import jax
import jax.numpy as jnp
from jax import lax
from jax.experimental import pallas as pl
from jax.experimental.pallas import tpu as pltpu
from jax.sharding import PartitionSpec as P

EPSILON = 1e-05
F32 = jnp.float32
BF16 = jnp.bfloat16
VMEM = pl.BlockSpec(memory_space=pltpu.VMEM)


def silu_slope(value):
    sigma = jax.nn.sigmoid(value)
    return sigma * (1.0 + value * (1.0 - sigma))


def times_transpose(left, right):
    return lax.dot_general(left, right, (((1,), (1,)), ((), ())), preferred_element_type=F32)


def first_contract(left, right):
    return lax.dot_general(left, right, (((0,), (0,)), ((), ())), preferred_element_type=F32)


def remote(src, dst, send, recv, device):
    return pltpu.make_async_remote_copy(
        src_ref=src,
        dst_ref=dst,
        send_sem=send,
        recv_sem=recv,
        device_id=device,
        device_id_type=pl.DeviceIdType.MESH,
    )


def greet(barrier, device):
    pl.semaphore_signal(barrier, inc=1, device_id=device, device_id_type=pl.DeviceIdType.MESH)


def near_barrier(bands, subs, band, me):
    barrier = pltpu.get_barrier_semaphore()
    for step in range(1, subs):
        greet(barrier, (band, lax.rem(me + step, subs)))

    @pl.when(band > 0)
    def _():
        for other in range(subs):
            greet(barrier, (band - 1, other))

    @pl.when(band < bands - 1)
    def _():
        for other in range(subs):
            greet(barrier, (band + 1, other))

    sides = jnp.minimum(band, 1) + jnp.minimum(bands - 1 - band, 1)
    pl.semaphore_wait(barrier, subs - 1 + subs * sides)


def place(subs):
    band, me = (lax.axis_index("band"), lax.axis_index("sub"))
    core = lax.rem(me, 2)
    return (band, me, core, me // 2, me + 1 - 2 * core, subs // 2)


def window_kernel(bands, subs, x_ref, o_ref, send, recv, local):
    band, me, core, chip, partner, chips = place(subs)
    near_barrier(bands, subs, band, me)
    own = pltpu.make_async_copy(x_ref, o_ref.at[1 + me], local)
    own.start()

    def push(src, slot, b, s, index):
        return remote(src, o_ref.at[slot], send.at[index], recv.at[slot], (b, s))

    def arrived(slot):
        push(x_ref, slot, band, partner, 0).wait_recv()

    across = [
        push(x_ref, 1 + me, band, 2 * lax.rem(chip + k, chips) + core, k - 1)
        for k in range(1, chips)
    ]
    pair = push(x_ref, 1 + me, band, partner, chips - 1)
    rising = (me == subs - 1) & (band < bands - 1)
    falling = (me == 0) & (band > 0)

    def up(k):
        return push(x_ref, 0, band + 1, 2 * k + 1, chips + k)

    def down(k):
        return push(x_ref, subs + 1, band - 1, 2 * k, 2 * chips + k)

    @pl.when(rising)
    def _():
        for k in range(chips):
            up(k).start()

    @pl.when(falling)
    def _():
        for k in range(chips):
            down(k).start()

    for copy in across:
        copy.start()
    pair.start()
    relays = []
    for k in range(1, chips):
        source = lax.rem(chip + chips - k, chips)
        slot = 1 + 2 * source + core
        arrived(slot)
        relay = push(o_ref.at[slot], slot, band, partner, 3 * chips + k - 1)
        relay.start()
        relays.append(relay)

    below = (core == 1) & (band > 0)
    above = (core == 0) & (band < bands - 1)
    relay_below = push(o_ref.at[0], 0, band, partner, 4 * chips - 1)
    relay_above = push(o_ref.at[subs + 1], subs + 1, band, partner, 4 * chips)

    @pl.when(below)
    def _():
        arrived(0)
        relay_below.start()

    @pl.when(above)
    def _():
        arrived(subs + 1)
        relay_above.start()

    @pl.when(band == 0)
    def _():
        o_ref[0] = jnp.zeros(o_ref.shape[1:], o_ref.dtype)

    @pl.when(band == bands - 1)
    def _():
        o_ref[subs + 1] = jnp.zeros(o_ref.shape[1:], o_ref.dtype)

    arrived(1 + partner)
    for k in range(1, chips):
        source = lax.rem(chip + chips - k, chips)
        arrived(2 + 2 * source - core)

    @pl.when((core == 0) & (band > 0))
    def _():
        arrived(0)

    @pl.when((core == 1) & (band < bands - 1))
    def _():
        arrived(subs + 1)

    for copy in across + [pair] + relays:
        copy.wait_send()

    @pl.when(rising)
    def _():
        for k in range(chips):
            up(k).wait_send()

    @pl.when(falling)
    def _():
        for k in range(chips):
            down(k).wait_send()

    @pl.when(below)
    def _():
        relay_below.wait_send()

    @pl.when(above)
    def _():
        relay_above.wait_send()

    own.wait()


def fetch_window(block, bands, subs, ident):
    chips = subs // 2
    return pl.pallas_call(
        functools.partial(window_kernel, bands, subs),
        out_shape=jax.ShapeDtypeStruct((subs + 2,) + block.shape, block.dtype),
        in_specs=[VMEM],
        out_specs=VMEM,
        scratch_shapes=[
            pltpu.SemaphoreType.DMA((4 * chips + 1,)),
            pltpu.SemaphoreType.DMA((subs + 2,)),
            pltpu.SemaphoreType.DMA,
        ],
        compiler_params=pltpu.CompilerParams(collective_id=ident, has_side_effects=True),
        name=f"window{ident}",
    )(block)


def return_stream(
    bands, subs, work, g_ref, o_ref, pairbuf, stage, far, edge, send1, recv1, send2, far_sem, edge_sem
):
    band, me, core, chip, partner, chips = place(subs)
    order = list(range(1, chips)) + [chips, 0]

    def slot_of(step, which):
        if step == chips:
            return (1 - which) * (subs + 1)
        return 1 + 2 * lax.rem(chip + step, chips) + which

    swaps = {}
    for step in order:
        work(slot_of(step, 1 - core))
        swaps[step] = remote(
            g_ref.at[slot_of(step, 1 - core)],
            pairbuf.at[step],
            send1.at[step],
            recv1.at[step],
            (band, partner),
        )
        swaps[step].start()
        yield

    def combined(step):
        work(slot_of(step, core))
        swaps[step].wait_recv()
        return g_ref[slot_of(step, core)].astype(F32) + pairbuf[step].astype(F32)

    across = []
    for step in range(1, chips):
        stage[step - 1] = combined(step).astype(BF16)
        copy = remote(
            stage.at[step - 1],
            far.at[step - 1],
            send2.at[step - 1],
            far_sem.at[step - 1],
            (band, 2 * lax.rem(chip + step, chips) + core),
        )
        copy.start()
        across.append(copy)
        yield
    stage[chips - 1] = combined(chips).astype(BF16)

    def border(b, s):
        return remote(
            stage.at[chips - 1], edge.at[chip], send2.at[chips - 1], edge_sem.at[chip], (b, s)
        )

    below = (core == 1) & (band > 0)
    above = (core == 0) & (band < bands - 1)

    @pl.when(below)
    def _():
        border(band - 1, subs - 1).start()

    @pl.when(above)
    def _():
        border(band + 1, 0).start()

    yield
    total = combined(0)
    yield
    for step, copy in enumerate(across):
        copy.wait_recv()
        total = total + far[step].astype(F32)
    o_ref[...] = total

    def add_edges():
        extra = o_ref[...]
        for k in range(chips):
            remote(
                stage.at[chips - 1], edge.at[k], send2.at[chips - 1], edge_sem.at[k], (band, partner)
            ).wait_recv()
            extra = extra + edge[k].astype(F32)
        o_ref[...] = extra

    @pl.when((me == subs - 1) & (band < bands - 1))
    def _():
        add_edges()

    @pl.when((me == 0) & (band > 0))
    def _():
        add_edges()

    for step in order:
        swaps[step].wait_send()
    for copy in across:
        copy.wait_send()

    @pl.when(below)
    def _():
        border(band - 1, subs - 1).wait_send()

    @pl.when(above)
    def _():
        border(band + 1, 0).wait_send()


def return_kernel(bands, subs, *refs):
    band, me = (lax.axis_index("band"), lax.axis_index("sub"))
    near_barrier(bands, subs, band, me)
    for _ in return_stream(bands, subs, lambda slot: None, *refs):
        pass


def return_scratch(chips, block):
    dma = pltpu.SemaphoreType.DMA
    return [
        pltpu.VMEM((chips + 1,) + block, BF16),
        pltpu.VMEM((chips,) + block, BF16),
        pltpu.VMEM((chips,) + block, BF16),
        pltpu.VMEM((chips,) + block, BF16),
        dma((chips + 1,)),
        dma((chips + 1,)),
        dma((chips,)),
        dma((chips,)),
        dma((chips,)),
    ]


def return_window(slots, bands, subs, ident):
    chips = subs // 2
    block = slots.shape[1:]
    return pl.pallas_call(
        functools.partial(return_kernel, bands, subs),
        out_shape=jax.ShapeDtypeStruct(block, F32),
        in_specs=[VMEM],
        out_specs=VMEM,
        scratch_shapes=return_scratch(chips, block),
        compiler_params=pltpu.CompilerParams(collective_id=ident, has_side_effects=True),
        name=f"return{ident}",
    )(slots)


def sum_stream(
    bands, subs, v_ref, o_ref, r1, a1, r2, a2, r3, s1, q1, s2, q2, s3, q3, s4, q4, s5, q5, s6, q6
):
    band, me, core, chip, partner, chips = place(subs)
    half = chips * bands

    def part(which, step):
        return pl.ds(which * half + lax.rem(chip + step, chips) * bands, bands)

    order = list(range(1, chips)) + [0]
    swaps = {}
    for step in order:
        swaps[step] = remote(
            v_ref.at[part(1 - core, step)], r1.at[step], s1.at[step], q1.at[step], (band, partner)
        )
        swaps[step].start()
    waits = list(swaps.values())
    yield
    across = []
    for step in order:
        swaps[step].wait_recv()
        total = v_ref[part(core, step)].astype(F32) + r1[step].astype(F32)
        if step > 0:
            a1[step] = total.astype(BF16)
            copy = remote(
                a1.at[step],
                r2.at[step],
                s2.at[step],
                q2.at[step],
                (band, 2 * lax.rem(chip + step, chips) + core),
            )
            copy.start()
            across.append(copy)
    yield
    for step, copy in enumerate(across):
        copy.wait_recv()
        total = total + r2[step + 1].astype(F32)
    waits += across
    a2[...] = total.astype(BF16)
    spread = []
    for i in range(1, bands):
        goal = lax.rem(band + i, bands)
        copy = remote(a2.at[goal], r3.at[i], s3.at[i], q3.at[i], (goal, me))
        copy.start()
        spread.append(copy)
    yield
    total = a2[band].astype(F32)
    for i, copy in enumerate(spread):
        copy.wait_recv()
        total = total + r3[i + 1].astype(F32)
    waits += spread
    mine = core * half + chip * bands + band
    o_ref[mine] = total.astype(BF16)
    spread = []
    for i in range(1, bands):
        copy = remote(
            o_ref.at[mine], o_ref.at[mine], s4.at[i], q4.at[i], (lax.rem(band + i, bands), me)
        )
        copy.start()
        spread.append(copy)
    yield
    for copy in spread:
        copy.wait_recv()
    waits += spread
    across = []
    for step in range(1, chips):
        copy = remote(
            o_ref.at[part(core, 0)],
            o_ref.at[part(core, 0)],
            s5.at[step],
            q5.at[step],
            (band, 2 * lax.rem(chip + step, chips) + core),
        )
        copy.start()
        across.append(copy)
    relays = [
        remote(
            o_ref.at[part(core, 0)], o_ref.at[part(core, 0)], s6.at[0], q6.at[0], (band, partner)
        )
    ]
    relays[0].start()
    yield
    for step, copy in enumerate(across):
        copy.wait_recv()
        rows = part(core, chips - step - 1)
        relay = remote(
            o_ref.at[rows], o_ref.at[rows], s6.at[step + 1], q6.at[step + 1], (band, partner)
        )
        relay.start()
        relays.append(relay)
    yield
    for relay in relays:
        relay.wait_recv()
    for copy in waits + across + relays:
        copy.wait_send()


def sum_scratch(chips, bands, deep, latent):
    dma = pltpu.SemaphoreType.DMA
    return (
        [pltpu.VMEM((chips, bands, deep, latent), BF16)] * 3
        + [pltpu.VMEM((bands, deep, latent), BF16)] * 2
        + [dma((chips,))] * 4
        + [dma((bands,))] * 4
        + [dma((chips,))] * 4
    )


def tail_kernel(bands, subs, *refs):
    band, me = (lax.axis_index("band"), lax.axis_index("sub"))
    barrier = pltpu.get_barrier_semaphore()
    for step in range(1, subs):
        greet(barrier, (band, lax.rem(me + step, subs)))

    @pl.when(band > 0)
    def _():
        for other in range(subs):
            greet(barrier, (band - 1, other))

    @pl.when(band < bands - 1)
    def _():
        for other in range(subs):
            greet(barrier, (band + 1, other))

    for i in range(1, bands):
        goal = lax.rem(band + i, bands)

        @pl.when((goal != band + 1) & (goal != band - 1))
        def _():
            greet(barrier, (goal, me))

    sides = jnp.minimum(band, 1) + jnp.minimum(bands - 1 - band, 1)
    pl.semaphore_wait(barrier, subs + bands - 2 + (subs - 1) * sides)
    v_ref, index_ref, b_ref, hidden_ref, slope_ref, src_ref, embed_ref = refs[:7]
    src_out, edge_out, grid_out, slots, parts, total = refs[7:13]
    scratch = refs[13:]
    nodes = hidden_ref.shape[1]
    edges = index_ref.shape[1]
    total[...] = jnp.zeros_like(total)

    def work(slot):
        rows = lax.broadcasted_iota(jnp.int32, (nodes, edges), 0)
        picks = jnp.where(rows == index_ref[...] - slot * nodes, 1.0, 0.0).astype(BF16)
        grad = jnp.dot(picks, b_ref[...], preferred_element_type=F32).astype(BF16)
        total[...] += first_contract(hidden_ref[slot], grad)
        grad = times_transpose(grad, src_ref[...]) * slope_ref[slot].astype(F32)
        slots[slot] = times_transpose(embed_ref[...], grad.astype(BF16)).astype(BF16)

    edge = sum_stream(bands, subs, v_ref, edge_out, *scratch[:17])
    src = sum_stream(bands, subs, parts, src_out, *scratch[17:34])
    back = return_stream(bands, subs, work, slots, grid_out, *scratch[34:])
    next(edge)
    for _ in range(subs + 2):
        next(back)
        next(edge, True)
    deep = parts.shape[1]
    for i in range(parts.shape[0]):
        parts[i] = total[i * deep : (i + 1) * deep].astype(BF16)
    active = [src, back, edge]
    while active:
        active = [stream for stream in active if next(stream, True) is None]


def tail(edge_part, index, before_grad, hidden, slope, w_src, w_embed, bands, subs, ident):
    chips = subs // 2
    count = bands * subs
    latent = w_src.shape[0]
    slots, nodes, _ = hidden.shape
    block = (w_embed.shape[0], nodes)
    deep = latent // count
    shape = (count, deep, latent)
    src, edge, grid = pl.pallas_call(
        functools.partial(tail_kernel, bands, subs),
        out_shape=[jax.ShapeDtypeStruct(shape, BF16)] * 2 + [jax.ShapeDtypeStruct(block, F32)],
        in_specs=[VMEM] * 7,
        out_specs=[VMEM] * 3,
        scratch_shapes=[
            pltpu.VMEM((slots,) + block, BF16),
            pltpu.VMEM(shape, BF16),
            pltpu.VMEM((latent, latent), F32),
        ]
        + sum_scratch(chips, bands, deep, latent) * 2
        + return_scratch(chips, block),
        compiler_params=pltpu.CompilerParams(collective_id=ident, has_side_effects=True),
        name="tail",
    )(edge_part.reshape(shape), index, before_grad, hidden, slope, w_src, w_embed)
    return src.reshape(latent, latent), edge.reshape(latent, latent), grid


def encode_kernel(edges, g_ref, d_ref, m_ref, w_ref, a_ref, l_ref, n_ref, i_ref, h_ref):
    rows, latent = d_ref.shape
    before = g_ref[...].astype(F32).reshape(rows, edges, latent) + d_ref[...][:, None, :]
    before = before.reshape(rows * edges, latent)
    sigma = jax.nn.sigmoid(before)
    active = before * sigma
    l_ref[...] = (sigma + active * (1.0 - sigma)).astype(BF16)
    active = active.astype(BF16)
    a_ref[...] = active
    out = jnp.dot(active, w_ref[...], preferred_element_type=F32)
    out = out - jnp.mean(out, axis=-1, keepdims=True)
    inverse = 1.0 / jnp.sqrt(jnp.mean(out * out, axis=-1, keepdims=True) + EPSILON)
    out = out * inverse
    i_ref[...] = inverse
    n_ref[...] = out.astype(BF16)
    encoded = jnp.sum(out.reshape(rows, edges, latent), axis=1)
    h_ref[...] = (m_ref[...].astype(F32) + encoded * (1.0 / math.sqrt(edges))).astype(BF16)


def rows_spec(rows, width):
    return pl.BlockSpec((rows, width), lambda i: (i, 0))


def encode(gathered, dest, mesh_in, w_edge, edges, tile):
    rows, latent = dest.shape
    total = rows * edges
    wide = rows_spec(tile * edges, latent)
    return pl.pallas_call(
        functools.partial(encode_kernel, edges),
        grid=(rows // tile,),
        out_shape=[jax.ShapeDtypeStruct((total, latent), BF16)] * 3
        + [
            jax.ShapeDtypeStruct((total, 1), F32),
            jax.ShapeDtypeStruct((rows, latent), BF16),
        ],
        in_specs=[
            wide,
            rows_spec(tile, latent),
            rows_spec(tile, latent),
            pl.BlockSpec((latent, latent), lambda i: (0, 0)),
        ],
        out_specs=[wide] * 3 + [rows_spec(tile * edges, 1), rows_spec(tile, latent)],
        name="encode",
    )(gathered, dest, mesh_in, w_edge)


def decode_kernel(edges, u_ref, n_ref, i_ref, l_ref, w_ref, g_ref, b_ref):
    rows, latent = u_ref.shape
    upper = u_ref[...] * (1.0 / math.sqrt(edges))
    normed = n_ref[...].astype(F32).reshape(rows, edges, latent)
    both = jnp.mean(upper[:, None, :] * normed, axis=-1, keepdims=True)
    upper = upper - jnp.mean(upper, axis=-1, keepdims=True)
    grad = (upper[:, None, :] - normed * both).reshape(rows * edges, latent) * i_ref[...]
    grad = grad.astype(BF16)
    g_ref[...] = grad
    b_ref[...] = (times_transpose(grad, w_ref[...]) * l_ref[...].astype(F32)).astype(BF16)


def decode(mesh_grad, normed, inverse, slope, w_edge, edges, tile):
    rows, latent = mesh_grad.shape
    wide = rows_spec(tile * edges, latent)
    return pl.pallas_call(
        functools.partial(decode_kernel, edges),
        grid=(rows // tile,),
        out_shape=[jax.ShapeDtypeStruct((rows * edges, latent), BF16)] * 2,
        in_specs=[
            rows_spec(tile, latent),
            wide,
            rows_spec(tile * edges, 1),
            wide,
            pl.BlockSpec((latent, latent), lambda i: (0, 0)),
        ],
        out_specs=[wide] * 2,
        name="decode",
    )(mesh_grad, normed, inverse, slope, w_edge)


def one_hot(index, count):
    return (index[:, None] == lax.broadcasted_iota(jnp.int32, (1, count), 1)).astype(BF16)


def body(
    bands, subs,
    grid_x, mesh_in, w_embed, w_src, w_dst, w_edge, w_proc, w_recv, g2m_src, mesh_src, cotangent
):
    latent = w_src.shape[0]
    channels, nodes = grid_x.shape
    mesh_rows, enc_count = g2m_src.shape
    mesh_count = mesh_src.shape[1]
    slots = subs + 2
    band_index = lax.axis_index("band")

    x_window = fetch_window(grid_x, bands, subs, 0)
    hidden_pre = lax.dot_general(
        x_window, w_embed, (((1,), (0,)), ((), ())), preferred_element_type=F32
    ).reshape(slots * nodes, latent)
    hidden = jax.nn.silu(hidden_pre).astype(BF16)
    projected = jnp.dot(hidden, w_src, preferred_element_type=F32).astype(BF16)
    dest_term = jnp.dot(mesh_in, w_dst, preferred_element_type=F32)
    grid_local = (g2m_src - (band_index * (nodes * subs) - nodes)).reshape(-1)
    gathered = projected.at[grid_local].get(mode="promise_in_bounds")
    active, slope, normed, inverse, hidden_mesh = encode(
        gathered, dest_term, mesh_in, w_edge, enc_count, 16
    )
    query = jnp.dot(hidden_mesh, w_proc, preferred_element_type=F32).astype(BF16)
    receiver = jnp.dot(hidden_mesh, w_recv, preferred_element_type=F32)
    mesh_window = fetch_window(query, bands, subs, 1).reshape(slots * mesh_rows, latent)
    mesh_local = (mesh_src - (band_index * (mesh_rows * subs) - mesh_rows)).T.reshape(-1)
    picks = one_hot(mesh_local, slots * mesh_rows)
    mesh_before = jnp.dot(picks, mesh_window, preferred_element_type=F32)
    mesh_before = mesh_before.reshape(mesh_count, mesh_rows, latent) + receiver[None]
    summed = jnp.sum(jax.nn.silu(mesh_before), axis=0)
    mesh_out = (hidden_mesh.astype(F32) + summed / math.sqrt(mesh_count)).astype(BF16)
    upstream = cotangent.astype(F32)
    mesh_slope = (upstream / math.sqrt(mesh_count))[None] * silu_slope(mesh_before)
    receiver_grad = jnp.sum(mesh_slope, axis=0)
    query_window = first_contract(picks, mesh_slope.reshape(-1, latent).astype(BF16)).astype(BF16)
    query_grad = return_window(query_window.reshape(slots, mesh_rows, latent), bands, subs, 2)
    mesh_grad = upstream + times_transpose(query_grad.astype(BF16), w_proc)
    mesh_grad = mesh_grad + times_transpose(receiver_grad.astype(BF16), w_recv)
    norm_grad, before_grad = decode(mesh_grad, normed, inverse, slope, w_edge, enc_count, 16)
    edge_part = first_contract(active, norm_grad)
    src_grad, edge_grad, grid_grad = tail(
        edge_part.astype(BF16),
        grid_local[None, :],
        before_grad,
        hidden.reshape(slots, nodes, latent),
        silu_slope(hidden_pre).astype(BF16).reshape(slots, nodes, latent),
        w_src,
        w_embed,
        bands,
        subs,
        3,
    )
    return (mesh_out, grid_grad, src_grad.astype(F32), edge_grad.astype(F32))


def solution(mesh):
    nodes = P(("band", "sub"), None)
    placed = (P(None, ("band", "sub")), nodes) + (P(),) * 6 + (nodes,) * 3
    return jax.shard_map(
        functools.partial(body, mesh.shape["band"], mesh.shape["sub"]),
        mesh=mesh,
        in_specs=placed,
        out_specs=(nodes, P(None, ("band", "sub")), P(), P()),
        check_vma=False,
    )
```

```python
import functools
import math

import jax
import jax.numpy as jnp
from jax import lax
from jax.experimental import pallas as pl
from jax.experimental.pallas import tpu as pltpu
from jax.sharding import PartitionSpec as P

EPSILON = 1e-05
F32 = jnp.float32
BF16 = jnp.bfloat16
VMEM = pl.BlockSpec(memory_space=pltpu.VMEM)


def silu_slope(value):
    sigma = jax.nn.sigmoid(value)
    return sigma * (1.0 + value * (1.0 - sigma))


def times_transpose(left, right):
    return lax.dot_general(left, right, (((1,), (1,)), ((), ())), preferred_element_type=F32)


def first_contract(left, right):
    return lax.dot_general(left, right, (((0,), (0,)), ((), ())), preferred_element_type=F32)


def remote(src, dst, send, recv, device):
    return pltpu.make_async_remote_copy(
        src_ref=src,
        dst_ref=dst,
        send_sem=send,
        recv_sem=recv,
        device_id=device,
        device_id_type=pl.DeviceIdType.MESH,
    )


def greet(barrier, device):
    pl.semaphore_signal(barrier, inc=1, device_id=device, device_id_type=pl.DeviceIdType.MESH)


def near_barrier(bands, subs, band, me):
    barrier = pltpu.get_barrier_semaphore()
    for step in range(1, subs):
        greet(barrier, (band, lax.rem(me + step, subs)))

    @pl.when(band > 0)
    def _():
        for other in range(subs):
            greet(barrier, (band - 1, other))

    @pl.when(band < bands - 1)
    def _():
        for other in range(subs):
            greet(barrier, (band + 1, other))

    sides = jnp.minimum(band, 1) + jnp.minimum(bands - 1 - band, 1)
    pl.semaphore_wait(barrier, subs - 1 + subs * sides)


def place(subs):
    band, me = (lax.axis_index("band"), lax.axis_index("sub"))
    core = lax.rem(me, 2)
    return (band, me, core, me // 2, me + 1 - 2 * core, subs // 2)


def window_kernel(bands, subs, x_ref, o_ref, send, recv, local):
    band, me, core, chip, partner, chips = place(subs)
    near_barrier(bands, subs, band, me)
    own = pltpu.make_async_copy(x_ref, o_ref.at[1 + me], local)
    own.start()

    def push(src, slot, b, s, index):
        return remote(src, o_ref.at[slot], send.at[index], recv.at[slot], (b, s))

    def arrived(slot):
        push(x_ref, slot, band, partner, 0).wait_recv()

    across = [
        push(x_ref, 1 + me, band, 2 * lax.rem(chip + k, chips) + core, k - 1)
        for k in range(1, chips)
    ]
    pair = push(x_ref, 1 + me, band, partner, chips - 1)
    rising = (me == subs - 1) & (band < bands - 1)
    falling = (me == 0) & (band > 0)

    def up(k):
        return push(x_ref, 0, band + 1, 2 * k + 1, chips + k)

    def down(k):
        return push(x_ref, subs + 1, band - 1, 2 * k, 2 * chips + k)

    @pl.when(rising)
    def _():
        for k in range(chips):
            up(k).start()

    @pl.when(falling)
    def _():
        for k in range(chips):
            down(k).start()

    for copy in across:
        copy.start()
    pair.start()
    relays = []
    for k in range(1, chips):
        source = lax.rem(chip + chips - k, chips)
        slot = 1 + 2 * source + core
        arrived(slot)
        relay = push(o_ref.at[slot], slot, band, partner, 3 * chips + k - 1)
        relay.start()
        relays.append(relay)

    below = (core == 1) & (band > 0)
    above = (core == 0) & (band < bands - 1)
    relay_below = push(o_ref.at[0], 0, band, partner, 4 * chips - 1)
    relay_above = push(o_ref.at[subs + 1], subs + 1, band, partner, 4 * chips)

    @pl.when(below)
    def _():
        arrived(0)
        relay_below.start()

    @pl.when(above)
    def _():
        arrived(subs + 1)
        relay_above.start()

    @pl.when(band == 0)
    def _():
        o_ref[0] = jnp.zeros(o_ref.shape[1:], o_ref.dtype)

    @pl.when(band == bands - 1)
    def _():
        o_ref[subs + 1] = jnp.zeros(o_ref.shape[1:], o_ref.dtype)

    arrived(1 + partner)
    for k in range(1, chips):
        source = lax.rem(chip + chips - k, chips)
        arrived(2 + 2 * source - core)

    @pl.when((core == 0) & (band > 0))
    def _():
        arrived(0)

    @pl.when((core == 1) & (band < bands - 1))
    def _():
        arrived(subs + 1)

    for copy in across + [pair] + relays:
        copy.wait_send()

    @pl.when(rising)
    def _():
        for k in range(chips):
            up(k).wait_send()

    @pl.when(falling)
    def _():
        for k in range(chips):
            down(k).wait_send()

    @pl.when(below)
    def _():
        relay_below.wait_send()

    @pl.when(above)
    def _():
        relay_above.wait_send()

    own.wait()


def fetch_window(block, bands, subs, ident):
    chips = subs // 2
    return pl.pallas_call(
        functools.partial(window_kernel, bands, subs),
        out_shape=jax.ShapeDtypeStruct((subs + 2,) + block.shape, block.dtype),
        in_specs=[VMEM],
        out_specs=VMEM,
        scratch_shapes=[
            pltpu.SemaphoreType.DMA((4 * chips + 1,)),
            pltpu.SemaphoreType.DMA((subs + 2,)),
            pltpu.SemaphoreType.DMA,
        ],
        compiler_params=pltpu.CompilerParams(collective_id=ident, has_side_effects=True),
        name=f"window{ident}",
    )(block)


def return_stream(
    bands, subs, g_ref, o_ref, pairbuf, stage, far, edge, send1, recv1, send2, far_sem, edge_sem
):
    band, me, core, chip, partner, chips = place(subs)
    order = list(range(1, chips)) + [chips, 0]

    def slot_of(step, which):
        if step == chips:
            return (1 - which) * (subs + 1)
        return 1 + 2 * lax.rem(chip + step, chips) + which

    swaps = {}
    for step in order:
        swaps[step] = remote(
            g_ref.at[slot_of(step, 1 - core)],
            pairbuf.at[step],
            send1.at[step],
            recv1.at[step],
            (band, partner),
        )
        swaps[step].start()
    yield

    def combined(step):
        swaps[step].wait_recv()
        return g_ref[slot_of(step, core)].astype(F32) + pairbuf[step].astype(F32)

    across = []
    for step in range(1, chips):
        stage[step - 1] = combined(step).astype(BF16)
        copy = remote(
            stage.at[step - 1],
            far.at[step - 1],
            send2.at[step - 1],
            far_sem.at[step - 1],
            (band, 2 * lax.rem(chip + step, chips) + core),
        )
        copy.start()
        across.append(copy)
    stage[chips - 1] = combined(chips).astype(BF16)

    def border(b, s):
        return remote(
            stage.at[chips - 1], edge.at[chip], send2.at[chips - 1], edge_sem.at[chip], (b, s)
        )

    below = (core == 1) & (band > 0)
    above = (core == 0) & (band < bands - 1)

    @pl.when(below)
    def _():
        border(band - 1, subs - 1).start()

    @pl.when(above)
    def _():
        border(band + 1, 0).start()

    yield
    total = combined(0)
    for step, copy in enumerate(across):
        copy.wait_recv()
        total = total + far[step].astype(F32)
    o_ref[...] = total

    def add_edges():
        extra = o_ref[...]
        for k in range(chips):
            remote(
                stage.at[chips - 1], edge.at[k], send2.at[chips - 1], edge_sem.at[k], (band, partner)
            ).wait_recv()
            extra = extra + edge[k].astype(F32)
        o_ref[...] = extra

    @pl.when((me == subs - 1) & (band < bands - 1))
    def _():
        add_edges()

    @pl.when((me == 0) & (band > 0))
    def _():
        add_edges()

    for step in order:
        swaps[step].wait_send()
    for copy in across:
        copy.wait_send()

    @pl.when(below)
    def _():
        border(band - 1, subs - 1).wait_send()

    @pl.when(above)
    def _():
        border(band + 1, 0).wait_send()


def return_kernel(bands, subs, *refs):
    band, me = (lax.axis_index("band"), lax.axis_index("sub"))
    near_barrier(bands, subs, band, me)
    for _ in return_stream(bands, subs, *refs):
        pass


def return_scratch(chips, block):
    dma = pltpu.SemaphoreType.DMA
    return [
        pltpu.VMEM((chips + 1,) + block, BF16),
        pltpu.VMEM((chips,) + block, BF16),
        pltpu.VMEM((chips,) + block, BF16),
        pltpu.VMEM((chips,) + block, BF16),
        dma((chips + 1,)),
        dma((chips + 1,)),
        dma((chips,)),
        dma((chips,)),
        dma((chips,)),
    ]


def return_window(slots, bands, subs, ident):
    chips = subs // 2
    block = slots.shape[1:]
    return pl.pallas_call(
        functools.partial(return_kernel, bands, subs),
        out_shape=jax.ShapeDtypeStruct(block, F32),
        in_specs=[VMEM],
        out_specs=VMEM,
        scratch_shapes=return_scratch(chips, block),
        compiler_params=pltpu.CompilerParams(collective_id=ident, has_side_effects=True),
        name=f"return{ident}",
    )(slots)


def sum_stream(
    bands, subs, v_ref, o_ref, r1, a1, r2, a2, r3, s1, q1, s2, q2, s3, q3, s4, q4, s5, q5, s6, q6
):
    band, me, core, chip, partner, chips = place(subs)
    half = chips * bands

    def part(which, step):
        return pl.ds(which * half + lax.rem(chip + step, chips) * bands, bands)

    order = list(range(1, chips)) + [0]
    swaps = {}
    for step in order:
        swaps[step] = remote(
            v_ref.at[part(1 - core, step)], r1.at[step], s1.at[step], q1.at[step], (band, partner)
        )
        swaps[step].start()
    waits = list(swaps.values())
    yield
    across = []
    for step in order:
        swaps[step].wait_recv()
        total = v_ref[part(core, step)].astype(F32) + r1[step].astype(F32)
        if step > 0:
            a1[step] = total.astype(BF16)
            copy = remote(
                a1.at[step],
                r2.at[step],
                s2.at[step],
                q2.at[step],
                (band, 2 * lax.rem(chip + step, chips) + core),
            )
            copy.start()
            across.append(copy)
    yield
    for step, copy in enumerate(across):
        copy.wait_recv()
        total = total + r2[step + 1].astype(F32)
    waits += across
    a2[...] = total.astype(BF16)
    spread = []
    for i in range(1, bands):
        goal = lax.rem(band + i, bands)
        copy = remote(a2.at[goal], r3.at[i], s3.at[i], q3.at[i], (goal, me))
        copy.start()
        spread.append(copy)
    yield
    total = a2[band].astype(F32)
    for i, copy in enumerate(spread):
        copy.wait_recv()
        total = total + r3[i + 1].astype(F32)
    waits += spread
    mine = core * half + chip * bands + band
    o_ref[mine] = total.astype(BF16)
    spread = []
    for i in range(1, bands):
        copy = remote(
            o_ref.at[mine], o_ref.at[mine], s4.at[i], q4.at[i], (lax.rem(band + i, bands), me)
        )
        copy.start()
        spread.append(copy)
    yield
    for copy in spread:
        copy.wait_recv()
    waits += spread
    across = []
    for step in range(1, chips):
        copy = remote(
            o_ref.at[part(core, 0)],
            o_ref.at[part(core, 0)],
            s5.at[step],
            q5.at[step],
            (band, 2 * lax.rem(chip + step, chips) + core),
        )
        copy.start()
        across.append(copy)
    relays = [
        remote(
            o_ref.at[part(core, 0)], o_ref.at[part(core, 0)], s6.at[0], q6.at[0], (band, partner)
        )
    ]
    relays[0].start()
    yield
    for step, copy in enumerate(across):
        copy.wait_recv()
        rows = part(core, chips - step - 1)
        relay = remote(
            o_ref.at[rows], o_ref.at[rows], s6.at[step + 1], q6.at[step + 1], (band, partner)
        )
        relay.start()
        relays.append(relay)
    yield
    for relay in relays:
        relay.wait_recv()
    for copy in waits + across + relays:
        copy.wait_send()


def sum_scratch(chips, bands, deep, latent):
    dma = pltpu.SemaphoreType.DMA
    return (
        [pltpu.VMEM((chips, bands, deep, latent), BF16)] * 3
        + [pltpu.VMEM((bands, deep, latent), BF16)] * 2
        + [dma((chips,))] * 4
        + [dma((bands,))] * 4
        + [dma((chips,))] * 4
    )


def tail_kernel(bands, subs, streams, *refs):
    band, me = (lax.axis_index("band"), lax.axis_index("sub"))
    barrier = pltpu.get_barrier_semaphore()
    for step in range(1, subs):
        greet(barrier, (band, lax.rem(me + step, subs)))

    @pl.when(band > 0)
    def _():
        for other in range(subs):
            greet(barrier, (band - 1, other))

    @pl.when(band < bands - 1)
    def _():
        for other in range(subs):
            greet(barrier, (band + 1, other))

    for i in range(1, bands):
        goal = lax.rem(band + i, bands)

        @pl.when((goal != band + 1) & (goal != band - 1))
        def _():
            greet(barrier, (goal, me))

    sides = jnp.minimum(band, 1) + jnp.minimum(bands - 1 - band, 1)
    pl.semaphore_wait(barrier, subs + bands - 2 + (subs - 1) * sides)
    count = streams + 1
    ins, outs, scratch = (refs[:count], refs[count : 2 * count], refs[2 * count :])
    active = [
        sum_stream(bands, subs, ins[i], outs[i], *scratch[17 * i : 17 * i + 17])
        for i in range(streams)
    ]
    active.append(return_stream(bands, subs, ins[-1], outs[-1], *scratch[17 * streams :]))
    while active:
        active = [stream for stream in active if next(stream, True) is None]


def tail(values, slots, bands, subs, ident):
    chips = subs // 2
    count = bands * subs
    rows, latent = values[0].shape
    deep = rows // count
    block = slots.shape[1:]
    shape = (count, deep, latent)
    scratch = []
    for _ in values:
        scratch += sum_scratch(chips, bands, deep, latent)
    results = pl.pallas_call(
        functools.partial(tail_kernel, bands, subs, len(values)),
        out_shape=[jax.ShapeDtypeStruct(shape, BF16)] * len(values)
        + [jax.ShapeDtypeStruct(block, F32)],
        in_specs=[VMEM] * (len(values) + 1),
        out_specs=[VMEM] * (len(values) + 1),
        scratch_shapes=scratch + return_scratch(chips, block),
        compiler_params=pltpu.CompilerParams(collective_id=ident, has_side_effects=True),
        name="tail",
    )(*[value.reshape(shape) for value in values], slots)
    return [result.reshape(rows, latent) for result in results[:-1]] + [results[-1]]


def encode_kernel(edges, g_ref, d_ref, m_ref, w_ref, a_ref, l_ref, n_ref, i_ref, h_ref):
    rows, latent = d_ref.shape
    before = g_ref[...].astype(F32).reshape(rows, edges, latent) + d_ref[...][:, None, :]
    before = before.reshape(rows * edges, latent)
    sigma = jax.nn.sigmoid(before)
    active = before * sigma
    l_ref[...] = (sigma + active * (1.0 - sigma)).astype(BF16)
    active = active.astype(BF16)
    a_ref[...] = active
    out = jnp.dot(active, w_ref[...], preferred_element_type=F32)
    out = out - jnp.mean(out, axis=-1, keepdims=True)
    inverse = 1.0 / jnp.sqrt(jnp.mean(out * out, axis=-1, keepdims=True) + EPSILON)
    out = out * inverse
    i_ref[...] = inverse
    n_ref[...] = out.astype(BF16)
    encoded = jnp.sum(out.reshape(rows, edges, latent), axis=1)
    h_ref[...] = (m_ref[...].astype(F32) + encoded * (1.0 / math.sqrt(edges))).astype(BF16)


def rows_spec(rows, width):
    return pl.BlockSpec((rows, width), lambda i: (i, 0))


def encode(gathered, dest, mesh_in, w_edge, edges, tile):
    rows, latent = dest.shape
    total = rows * edges
    wide = rows_spec(tile * edges, latent)
    return pl.pallas_call(
        functools.partial(encode_kernel, edges),
        grid=(rows // tile,),
        out_shape=[jax.ShapeDtypeStruct((total, latent), BF16)] * 3
        + [
            jax.ShapeDtypeStruct((total, 1), F32),
            jax.ShapeDtypeStruct((rows, latent), BF16),
        ],
        in_specs=[
            wide,
            rows_spec(tile, latent),
            rows_spec(tile, latent),
            pl.BlockSpec((latent, latent), lambda i: (0, 0)),
        ],
        out_specs=[wide] * 3 + [rows_spec(tile * edges, 1), rows_spec(tile, latent)],
        name="encode",
    )(gathered, dest, mesh_in, w_edge)


def decode_kernel(edges, u_ref, n_ref, i_ref, l_ref, w_ref, g_ref, b_ref):
    rows, latent = u_ref.shape
    upper = u_ref[...] * (1.0 / math.sqrt(edges))
    normed = n_ref[...].astype(F32).reshape(rows, edges, latent)
    both = jnp.mean(upper[:, None, :] * normed, axis=-1, keepdims=True)
    upper = upper - jnp.mean(upper, axis=-1, keepdims=True)
    grad = (upper[:, None, :] - normed * both).reshape(rows * edges, latent) * i_ref[...]
    grad = grad.astype(BF16)
    g_ref[...] = grad
    b_ref[...] = (times_transpose(grad, w_ref[...]) * l_ref[...].astype(F32)).astype(BF16)


def decode(mesh_grad, normed, inverse, slope, w_edge, edges, tile):
    rows, latent = mesh_grad.shape
    wide = rows_spec(tile * edges, latent)
    return pl.pallas_call(
        functools.partial(decode_kernel, edges),
        grid=(rows // tile,),
        out_shape=[jax.ShapeDtypeStruct((rows * edges, latent), BF16)] * 2,
        in_specs=[
            rows_spec(tile, latent),
            wide,
            rows_spec(tile * edges, 1),
            wide,
            pl.BlockSpec((latent, latent), lambda i: (0, 0)),
        ],
        out_specs=[wide] * 2,
        name="decode",
    )(mesh_grad, normed, inverse, slope, w_edge)


def one_hot(index, count):
    return (index[:, None] == lax.broadcasted_iota(jnp.int32, (1, count), 1)).astype(BF16)


def body(
    bands, subs,
    grid_x, mesh_in, w_embed, w_src, w_dst, w_edge, w_proc, w_recv, g2m_src, mesh_src, cotangent
):
    latent = w_src.shape[0]
    channels, nodes = grid_x.shape
    mesh_rows, enc_count = g2m_src.shape
    mesh_count = mesh_src.shape[1]
    slots = subs + 2
    band_index = lax.axis_index("band")

    x_window = fetch_window(grid_x, bands, subs, 0)
    hidden_pre = lax.dot_general(
        x_window, w_embed, (((1,), (0,)), ((), ())), preferred_element_type=F32
    ).reshape(slots * nodes, latent)
    hidden = jax.nn.silu(hidden_pre).astype(BF16)
    projected = jnp.dot(hidden, w_src, preferred_element_type=F32).astype(BF16)
    dest_term = jnp.dot(mesh_in, w_dst, preferred_element_type=F32)
    grid_local = (g2m_src - (band_index * (nodes * subs) - nodes)).reshape(-1)
    gathered = projected.at[grid_local].get(mode="promise_in_bounds")
    active, slope, normed, inverse, hidden_mesh = encode(
        gathered, dest_term, mesh_in, w_edge, enc_count, 16
    )
    query = jnp.dot(hidden_mesh, w_proc, preferred_element_type=F32).astype(BF16)
    receiver = jnp.dot(hidden_mesh, w_recv, preferred_element_type=F32)
    mesh_window = fetch_window(query, bands, subs, 1).reshape(slots * mesh_rows, latent)
    mesh_local = (mesh_src - (band_index * (mesh_rows * subs) - mesh_rows)).T.reshape(-1)
    picks = one_hot(mesh_local, slots * mesh_rows)
    mesh_before = jnp.dot(picks, mesh_window, preferred_element_type=F32)
    mesh_before = mesh_before.reshape(mesh_count, mesh_rows, latent) + receiver[None]
    summed = jnp.sum(jax.nn.silu(mesh_before), axis=0)
    mesh_out = (hidden_mesh.astype(F32) + summed / math.sqrt(mesh_count)).astype(BF16)
    upstream = cotangent.astype(F32)
    mesh_slope = (upstream / math.sqrt(mesh_count))[None] * silu_slope(mesh_before)
    receiver_grad = jnp.sum(mesh_slope, axis=0)
    query_window = first_contract(picks, mesh_slope.reshape(-1, latent).astype(BF16)).astype(BF16)
    query_grad = return_window(query_window.reshape(slots, mesh_rows, latent), bands, subs, 2)
    mesh_grad = upstream + times_transpose(query_grad.astype(BF16), w_proc)
    mesh_grad = mesh_grad + times_transpose(receiver_grad.astype(BF16), w_recv)
    norm_grad, before_grad = decode(mesh_grad, normed, inverse, slope, w_edge, enc_count, 16)
    edge_part = first_contract(active, norm_grad)
    window_grad = first_contract(one_hot(grid_local, slots * nodes), before_grad).astype(BF16)
    src_part = first_contract(hidden, window_grad)
    hidden_grad = (times_transpose(window_grad, w_src) * silu_slope(hidden_pre)).astype(BF16)
    grid_part = lax.dot_general(
        w_embed,
        hidden_grad.reshape(slots, nodes, latent),
        (((1,), (2,)), ((), ())),
        preferred_element_type=F32,
    )
    grid_part = jnp.swapaxes(grid_part, 0, 1).astype(BF16)
    src_grad, edge_grad, grid_grad = tail(
        [src_part.astype(BF16), edge_part.astype(BF16)], grid_part, bands, subs, 3
    )
    return (mesh_out, grid_grad, src_grad.astype(F32), edge_grad.astype(F32))


def solution(mesh):
    nodes = P(("band", "sub"), None)
    placed = (P(None, ("band", "sub")), nodes) + (P(),) * 6 + (nodes,) * 3
    return jax.shard_map(
        functools.partial(body, mesh.shape["band"], mesh.shape["sub"]),
        mesh=mesh,
        in_specs=placed,
        out_specs=(nodes, P(None, ("band", "sub")), P(), P()),
        check_vma=False,
    )
```
